32 devices in a mesh: py: 8 (over y, x, core), pz: 4 (over z).
Axes of the slice: x: 2, y: 2, z: 4, core: 2. Of those that a mesh axis runs over, the one named last changes fastest.
Arguments:
- velocity: float32 [3, 320, 320, 320], P(None, 'py', 'pz'), may hold values from -12 to 12
Outputs:
- filtered_velocity: float32 [3, 128, 128, 128], P(None, 'py', 'pz')
- subgrid_stress: float32 [6, 128, 128, 128], P(None, 'py', 'pz')
The draws below stay inside these ranges and needn't reach their ends.
All inputs are finite; a program needn't handle non-finite values.
Results may differ from the reference program's by a relative error of at most 0.000082.
Values sent between devices are 32-bit elements; how exact they have to be, the bound alone decides.
A program may use at most 128 MiB of HBM per device.

```python
import math
import jax
import jax.numpy as jnp

N = 320
M = 128


def block_levels(own_key, shape, pieces, least, largest):
    factor_of = 1.0
    for axis_at, parts in pieces:
        heights = jax.random.uniform(jax.random.fold_in(jax.random.fold_in(own_key, 6), axis_at), (parts,), jnp.float32, least / len(pieces), largest / len(pieces))
        factor_of = factor_of * jnp.repeat(jnp.exp(heights), shape[axis_at] // parts).reshape((-1,) + (1,) * (len(shape) - 1 - axis_at))
    return factor_of


def normal_values(rng, shape, spread, reach, shards=(), kind=jnp.bfloat16):
    drawn = jax.random.normal(rng, shape, jnp.float32) * spread
    if len(shards) > 0:
        drawn = block_levels(rng, shape, shards, -0.22, 0.18) * drawn
    return jnp.clip(drawn, min=-reach, max=reach).astype(kind)


def setup_inputs(seed: int = 0) -> dict:
    keys = jax.random.split(jax.random.key(seed), 2)
    return {
        "velocity": normal_values(keys[0], (3, N, N, N), 2.0, 12.0, ((1, 8), (2, 4)), jnp.float32),
    }


factor_pairs = ((0, 0), (0, 1), (0, 2), (1, 1), (1, 2), (2, 2))


def kept_indices():
    return jnp.concatenate([jnp.arange(M // 2, dtype=jnp.int32), jnp.arange(N - M // 2, N, dtype=jnp.int32)])


def filter_values():
    half_modes = M // 2
    signed_modes = jnp.concatenate([jnp.arange(half_modes, dtype=jnp.int32), jnp.arange(half_modes, dtype=jnp.int32) - half_modes])
    wave_numbers = signed_modes.astype(jnp.float32)
    squares = wave_numbers[:, None, None] ** 2 + wave_numbers[None, :, None] ** 2 + wave_numbers[None, None, :] ** 2
    valid_modes = signed_modes != -half_modes
    retained = valid_modes[:, None, None] & valid_modes[None, :, None] & valid_modes[None, None, :]
    filter_width = 2.0 * math.pi / M
    return jnp.where(retained, jnp.exp(-squares * (filter_width * filter_width / 24.0)), 0.0).astype(jnp.float32)


def filtered_field(fine_field, gain_table, kept_modes):
    spectrum = jnp.take(jnp.fft.fft(fine_field, axis=2), kept_modes, axis=2)
    spectrum = jnp.take(jnp.fft.fft(spectrum, axis=1), kept_modes, axis=1)
    spectrum = jnp.take(jnp.fft.fft(spectrum, axis=0), kept_modes, axis=0)
    coarse = jnp.real(jnp.fft.ifftn(spectrum * gain_table)) * (float(M) ** 3 / float(N) ** 3)
    return jnp.transpose(coarse, (1, 2, 0)).astype(jnp.float32)


def reference(velocity):
    gain_table = filter_values()
    kept_modes = kept_indices()
    coarse = [filtered_field(velocity[component], gain_table, kept_modes) for component in range(3)]
    products = [filtered_field(velocity[left_index] * velocity[right_index], gain_table, kept_modes) for left_index, right_index in factor_pairs]
    filtered = jnp.stack(coarse)
    stress = jnp.stack([products[position] - coarse[left_index] * coarse[right_index] for position, (left_index, right_index) in enumerate(factor_pairs)])
    return filtered, stress
```

```python
import functools
import math

import jax
import jax.numpy as jnp
import ml_dtypes
import numpy as np
from jax import lax
from jax.experimental import pallas as pl
from jax.experimental.pallas import tpu as pltpu
from jax.sharding import PartitionSpec as P

M = 128

factor_pairs = ((0, 0), (0, 1), (0, 2), (1, 1), (1, 2), (2, 2))
fields_count = 9
LANES = 128


def line_filter(fine, coarse):
    half = coarse // 2
    modes = np.arange(1, half)
    width = 2.0 * math.pi / coarse
    gain = np.exp(-(modes.astype(np.float64) ** 2) * (width * width / 24.0))
    turns = np.arange(coarse)[:, None] * fine - np.arange(fine)[None, :] * coarse
    period = fine * coarse
    matrix = np.ones((coarse, fine))
    for mode, weight in zip(modes, gain):
        matrix += 2.0 * weight * np.cos(2.0 * math.pi * ((mode * turns) % period) / period)
    return (matrix / fine).astype(np.float32)


def halves(matrix):
    top = matrix.astype(ml_dtypes.bfloat16)
    return top, (matrix - top.astype(np.float32)).astype(ml_dtypes.bfloat16)


def split(value):
    top = value.astype(jnp.bfloat16)
    return top, (value - top.astype(jnp.float32)).astype(jnp.bfloat16)


def dot(left, right):
    return jnp.dot(left, right, preferred_element_type=jnp.float32)


def rows_times(value, table):
    width = table.shape[1] // 2
    top, rest = split(value)
    both = dot(top, table)
    return both[:, :width] + both[:, width:] + dot(rest, table[:, :width])


def kernel(
    rows, columns, velocity, third, first, second, filtered, stress,
    fine, lines, send_a, recv_a, send_b, recv_b, send_c, recv_c,
    load_sem, send_a_sem, recv_a_sem, send_b_sem, recv_b_sem, send_c_sem, recv_c_sem,
):
    me_y = lax.axis_index("py")
    me_z = lax.axis_index("pz")
    _, _, blocks, near, fine_points = fine.shape
    depth = rows * blocks
    block, band = M // columns, M // rows
    share = block // rows
    slots = send_b.shape[0]
    MESH = pl.DeviceIdType.MESH

    for c in range(3):

        def load(b, carry):
            pltpu.make_async_copy(
                velocity.at[c, :, b, :], fine.at[c, b % rows, b // rows], load_sem.at[c]
            ).start()
            return carry

        lax.fori_loop(0, depth, load, 0)

    barrier = pltpu.get_barrier_semaphore()
    for k in range(1, columns):
        pl.semaphore_signal(
            barrier, inc=1, device_id=(me_y, (me_z + k) % columns), device_id_type=MESH
        )
    for j in range(1, rows):
        pl.semaphore_signal(
            barrier, inc=1, device_id=((me_y + j) % rows, me_z), device_id_type=MESH
        )
    pl.semaphore_wait(barrier, columns + rows - 2)

    def copy_a(f, j):
        return pltpu.make_async_remote_copy(
            src_ref=send_a.at[f, j - 1],
            dst_ref=recv_a.at[f, :, pl.ds(pl.multiple_of(me_y * near, 8), near)],
            send_sem=send_a_sem.at[f, j - 1],
            recv_sem=recv_a_sem.at[f, j - 1],
            device_id=((me_y + j) % rows, me_z),
            device_id_type=MESH,
        )

    def copy_b(f, k):
        return pltpu.make_async_remote_copy(
            src_ref=send_b.at[f % slots, pl.ds((me_z + k) % columns * share, share)],
            dst_ref=recv_b.at[f, :, pl.ds(pl.multiple_of(me_z * depth, 8), depth)],
            send_sem=send_b_sem.at[f, k - 1],
            recv_sem=recv_b_sem.at[f, k - 1],
            device_id=(me_y, (me_z + k) % columns),
            device_id_type=MESH,
        )

    def copy_c(f, j):
        return pltpu.make_async_remote_copy(
            src_ref=send_c.at[f, (me_y + j) % rows],
            dst_ref=recv_c.at[f, pl.ds(me_y, 1)],
            send_sem=send_c_sem.at[f, j - 1],
            recv_sem=recv_c_sem.at[f, j - 1],
            device_id=((me_y + j) % rows, me_z),
            device_id_type=MESH,
        )

    def pair_of(f):
        return f // 6 + f // 8, f - 3 - 2 * (f // 6) - f // 8

    def contract_third(f, product):
        if product:
            left, right = pair_of(f)
        else:
            left = right = f

        def piece(r, carry):
            value = fine[left, r]
            if product:
                value = value * fine[right, r]
            value = value.reshape(blocks * near, fine_points)
            lines[r] = rows_times(value, third[r]).reshape(blocks, near, LANES)
            return carry

        lax.fori_loop(0, rows, piece, 0)

        group = lax.broadcasted_iota(jnp.int32, (near, LANES), 1) % rows
        masks = [group == (me_y + r) % rows for r in range(rows)]

        def regroup(q, carry):
            parts = [lines[r, q] for r in range(rows)]
            for j in range(rows):
                out = parts[-1]
                for r in range(rows - 1):
                    out = jnp.where(masks[(j + r) % rows], parts[r], out)
                if j == 0:
                    recv_a[f, q, pl.ds(pl.multiple_of(me_y * near, 8), near)] = out
                else:
                    send_a[f, j - 1, q] = out
            return carry

        lax.fori_loop(0, blocks, regroup, 0)
        for j in range(1, rows):
            copy_a(f, j).start()

    def table_times(table, value):
        top, rest = split(value)
        both = dot(table, top)
        return both[:M] + both[M:] + dot(table[:M], rest)

    def contract_first(f, reuse):
        for j in range(1, rows):
            copy_a(f, j).wait_recv()
        if reuse:
            for k in range(1, columns):
                copy_b(f - slots, k).wait_send()
        slot = f % slots

        def piece(h, carry):
            value = jnp.concatenate([recv_a[f, 2 * h + i] for i in range(2)], axis=1)
            out = table_times(first[...], value)
            for i in range(2):
                turned = out[:, i * LANES : (i + 1) * LANES].T.reshape(M // rows, rows, M)
                send_b[slot, :, pl.ds(pl.multiple_of((2 * h + i) * rows, 8), rows)] = turned
            return carry

        lax.fori_loop(0, blocks // 2, piece, 0)
        for k in range(1, columns):
            copy_b(f, k).start()
        recv_b[f, :, pl.ds(pl.multiple_of(me_z * depth, 8), depth)] = send_b[
            slot, pl.ds(me_z * share, share)
        ]

    def contract_second(f):
        for k in range(1, columns):
            copy_b(f, k).wait_recv()
        for h in range(share // 2):
            value = jnp.concatenate([recv_b[f, 2 * h + i] for i in range(2)], axis=1)
            out = table_times(second[...], value)
            for i in range(2):
                part = out[:, i * LANES : (i + 1) * LANES]
                for d in range(rows):
                    send_c[f, d, 0, 2 * h + i] = part[d * band : (d + 1) * band]
        for j in range(1, rows):
            copy_c(f, j).start()
        recv_c[f, me_y] = send_c[f, me_y, 0]

    def place(f, product):
        for j in range(1, rows):
            copy_c(f, j).wait_recv()
        whole = recv_c.at[f].reshape(rows * share * band, M)

        def line(m, carry):
            out = whole[pl.ds(m, block, stride=band), :]
            if product:
                left, right = pair_of(f)
                stress[f - 3, m] = out - filtered[left, m] * filtered[right, m]
            else:
                filtered[f, m] = out
            return carry

        lax.fori_loop(0, band, line, 0)

    def loop(start, stop, *work):
        def body(f, carry):
            for one in work:
                one(f)
            return carry

        lax.fori_loop(start, stop, body, 0)

    def loaded(c):
        pltpu.make_async_copy(fine.at[c], fine.at[c], load_sem.at[c]).wait()

    loop(0, 3, loaded, lambda f: contract_third(f, False))
    loop(3, fields_count, lambda f: contract_third(f, True))
    loop(0, 2, lambda f: contract_first(f, False))
    loop(2, slots, lambda f: contract_first(f, False), lambda f: contract_second(f - 2))
    loop(slots, fields_count, lambda f: contract_first(f, True), lambda f: contract_second(f - 2))
    loop(fields_count - 2, fields_count, contract_second)
    loop(0, 3, lambda f: place(f, False))
    loop(3, fields_count, lambda f: place(f, True))

    def finish(f):
        for j in range(1, rows):
            copy_a(f, j).wait_send()
            copy_c(f, j).wait_send()

    loop(0, fields_count, finish)

    def drain(f):
        for k in range(1, columns):
            copy_b(f, k).wait_send()

    loop(fields_count - slots, fields_count, drain)


def tables(fine, rows, columns):
    matrix = line_filter(fine, M)
    depth = fine // columns
    block = M // columns
    share = block // rows
    top, rest = halves(matrix)
    spot, group = np.arange(M) // rows, np.arange(M) % rows
    third = []
    for r in range(rows):
        order = spot // share * block + (group - r) % rows * share + spot % share
        third.append(np.concatenate([top.T[:, order], rest.T[:, order]], axis=1))
    first = np.concatenate([top, rest])
    second = []
    point = np.arange(fine)
    for y in range(rows):
        order = point // rows * rows + (point - y) % rows
        second.append(np.concatenate([top[:, order], rest[:, order]]))
    return np.stack(third), first, np.stack(second)


def kernel_shards(velocity):
    rows, columns = lax.axis_size("py"), lax.axis_size("pz")
    me_y = lax.axis_index("py")
    _, near, depth, fine = velocity.shape
    blocks = depth // rows
    block, band = M // columns, M // rows
    share = block // rows
    slots = 3
    third, first, second = tables(fine, rows, columns)
    second = lax.dynamic_slice(jnp.asarray(second), (me_y, 0, 0), (1, 2 * M, fine))[0]
    vmem = pl.BlockSpec(memory_space=pltpu.VMEM)
    dma = pltpu.SemaphoreType.DMA
    f32 = jnp.float32
    return pl.pallas_call(
        functools.partial(kernel, rows, columns),
        out_shape=(
            jax.ShapeDtypeStruct((3, band, block, M), f32),
            jax.ShapeDtypeStruct((6, band, block, M), f32),
        ),
        in_specs=[pl.BlockSpec(memory_space=pl.ANY), vmem, vmem, vmem],
        out_specs=(vmem, vmem),
        scratch_shapes=[
            pltpu.VMEM((3, rows, blocks, near, fine), f32),
            pltpu.VMEM((rows, blocks, near, LANES), f32),
            pltpu.VMEM((fields_count, rows - 1, blocks, near, LANES), f32),
            pltpu.VMEM((fields_count, blocks, rows * near, LANES), f32),
            pltpu.VMEM((slots, columns * share, depth, M), f32),
            pltpu.VMEM((fields_count, share, columns * depth, M), f32),
            pltpu.VMEM((fields_count, rows, 1, share, band, M), f32),
            pltpu.VMEM((fields_count, rows, share, band, M), f32),
            dma((3,)),
            dma((fields_count, rows - 1)),
            dma((fields_count, rows - 1)),
            dma((fields_count, columns - 1)),
            dma((fields_count, columns - 1)),
            dma((fields_count, rows - 1)),
            dma((fields_count, rows - 1)),
        ],
        compiler_params=pltpu.CompilerParams(
            collective_id=0, has_side_effects=True, vmem_limit_bytes=67_000_000
        ),
    )(velocity, jnp.asarray(third), jnp.asarray(first), second)


def plain_shards(velocity):
    matrix = jnp.asarray(line_filter(velocity.shape[3], M))
    components = [velocity[component] for component in range(3)]
    fields = jnp.stack(components + [components[a] * components[b] for a, b in factor_pairs])
    high = lax.Precision.HIGHEST
    third = jnp.einsum("fabk,mk->fabm", fields, matrix, precision=high)
    third = lax.all_to_all(third, "pz", split_axis=3, concat_axis=2, tiled=True)
    second = jnp.einsum("fabm,nb->fanm", third, matrix, precision=high)
    second = lax.all_to_all(second, "py", split_axis=2, concat_axis=1, tiled=True)
    coarse = jnp.einsum("fanm,pa->fnmp", second, matrix, precision=high)
    stress = jnp.stack(
        [coarse[3 + p] - coarse[a] * coarse[b] for p, (a, b) in enumerate(factor_pairs)]
    )
    return coarse[:3], stress


def shards(velocity):
    rows, columns = lax.axis_size("py"), lax.axis_size("pz")
    _, lines, depth, fine = velocity.shape
    whole_tiles = (
        M == LANES
        and rows % 8 == 0
        and lines % 8 == 0
        and depth % (2 * rows) == 0
        and M % (2 * rows * columns) == 0
        and (M // rows) % 8 == 0
    )
    return kernel_shards(velocity) if whole_tiles else plain_shards(velocity)


def solution(mesh):
    placed = P(None, "py", "pz", None)
    return jax.shard_map(
        shards, mesh=mesh, in_specs=(placed,), out_specs=(placed, placed), check_vma=False
    )
```

```python
import functools
import math

import jax
import jax.numpy as jnp
import ml_dtypes
import numpy as np
from jax import lax
from jax.experimental import pallas as pl
from jax.experimental.pallas import tpu as pltpu
from jax.sharding import PartitionSpec as P

M = 128

factor_pairs = ((0, 0), (0, 1), (0, 2), (1, 1), (1, 2), (2, 2))
fields_count = 9
LANES = 128


def line_filter(fine, coarse):
    half = coarse // 2
    modes = np.arange(1, half)
    width = 2.0 * math.pi / coarse
    gain = np.exp(-(modes.astype(np.float64) ** 2) * (width * width / 24.0))
    turns = np.arange(coarse)[:, None] * fine - np.arange(fine)[None, :] * coarse
    period = fine * coarse
    matrix = np.ones((coarse, fine))
    for mode, weight in zip(modes, gain):
        matrix += 2.0 * weight * np.cos(2.0 * math.pi * ((mode * turns) % period) / period)
    return (matrix / fine).astype(np.float32)


def halves(matrix):
    top = matrix.astype(ml_dtypes.bfloat16)
    return top, (matrix - top.astype(np.float32)).astype(ml_dtypes.bfloat16)


def split(value):
    top = value.astype(jnp.bfloat16)
    return top, (value - top.astype(jnp.float32)).astype(jnp.bfloat16)


def dot(left, right):
    return jnp.dot(left, right, preferred_element_type=jnp.float32)


def rows_times(value, table):
    width = table.shape[1] // 2
    top, rest = split(value)
    both = dot(top, table)
    return both[:, :width] + both[:, width:] + dot(rest, table[:, :width])


def flip(me, bits):
    out, weight = me, 1
    while weight <= bits:
        if bits & weight:
            out = out + weight - 2 * weight * (me // weight % 2)
        weight *= 2
    return out


def flip_by(value, bits, rows):
    out, weight = value, 1
    while weight < rows:
        bit = bits // weight % 2
        out = out + bit * (weight - 2 * weight * (value // weight % 2))
        weight *= 2
    return out


def spread(rows, mode):
    step = rows // 2 if mode == 0 else rows // 4
    return step, [(j, j // step % 2, j // (2 * step) * step + j % step) for j in range(rows)]


def kernel(
    rows, columns, velocity, third_table, first_table, base_table, filtered, stress,
    third, first, base, second, fine, lines, send_a, recv_a, send_p, recv_p, send_b, recv_b, send_c, recv_c,
    table_sem, load_sem, send_a_sem, recv_a_sem, send_p_sem, recv_p_sem,
    send_b_sem, recv_b_sem, send_c_sem, recv_c_sem,
):
    me_y = lax.axis_index("py")
    me_z = lax.axis_index("pz")
    _, _, blocks, near, fine_points = fine.shape
    depth = rows * blocks
    block, band = M // columns, M // rows
    share = block // rows
    slots_a, slots_p, slots_b = send_a.shape[0], send_p.shape[0], send_b.shape[0]
    MESH = pl.DeviceIdType.MESH

    steps_of = [spread(rows, mode)[0] for mode in range(2)]
    table_copies = [
        pltpu.make_async_copy(third_table, third, table_sem.at[0]),
        pltpu.make_async_copy(base_table, base, table_sem.at[1]),
    ] + [
        pltpu.make_async_copy(
            first_table.at[mode, me_y // steps_of[mode] % 2], first.at[mode], table_sem.at[2 + mode]
        )
        for mode in range(2)
    ]
    for copy in table_copies:
        copy.start()

    for c in range(3):

        def load(b, carry):
            pltpu.make_async_copy(
                velocity.at[c, :, b, :], fine.at[c, b % rows, b // rows], load_sem.at[c]
            ).start()
            return carry

        lax.fori_loop(0, depth, load, 0)

    barrier = pltpu.get_barrier_semaphore()
    for k in range(1, columns):
        pl.semaphore_signal(
            barrier, inc=1, device_id=(me_y, (me_z + k) % columns), device_id_type=MESH
        )
    for j in range(1, rows):
        pl.semaphore_signal(barrier, inc=1, device_id=(flip(me_y, j), me_z), device_id_type=MESH)
    pl.semaphore_wait(barrier, columns + rows - 2)

    def own_lines(mode):
        step = steps_of[mode]
        at = me_y // (2 * step) * step + me_y % step
        return pl.ds(pl.multiple_of(at * near, 8), near)

    def copies_a(f, mode, side):
        step, tiles = spread(rows, mode)
        return [
            pltpu.make_async_remote_copy(
                src_ref=send_a.at[f % slots_a, side, u - 1],
                dst_ref=recv_a.at[f, side, :, own_lines(mode)],
                send_sem=send_a_sem.at[f, side, u - 1],
                recv_sem=recv_a_sem.at[f, side, u - 1],
                device_id=(flip(me_y, j - side * step), me_z),
                device_id_type=MESH,
            )
            for j, s, u in tiles
            if s == side and u > 0
        ]

    def copy_p(f, mode):
        step, _ = spread(rows, mode)
        return pltpu.make_async_remote_copy(
            src_ref=send_p.at[f % slots_p],
            dst_ref=recv_p.at[f],
            send_sem=send_p_sem.at[f],
            recv_sem=recv_p_sem.at[f],
            device_id=(flip(me_y, step), me_z),
            device_id_type=MESH,
        )

    def copy_b(f, k):
        return pltpu.make_async_remote_copy(
            src_ref=send_b.at[f % slots_b, pl.ds((me_z + k) % columns * share, share)],
            dst_ref=recv_b.at[f, :, pl.ds(pl.multiple_of(me_z * depth, 8), depth)],
            send_sem=send_b_sem.at[f, k - 1],
            recv_sem=recv_b_sem.at[f, k - 1],
            device_id=(me_y, (me_z + k) % columns),
            device_id_type=MESH,
        )

    def copy_c(f, j):
        return pltpu.make_async_remote_copy(
            src_ref=send_c.at[f, pl.ds(flip(me_y, j), 1)],
            dst_ref=recv_c.at[f, pl.ds(me_y, 1)],
            send_sem=send_c_sem.at[f, j - 1],
            recv_sem=recv_c_sem.at[f, j - 1],
            device_id=(flip(me_y, j), me_z),
            device_id_type=MESH,
        )

    def pair_of(f):
        return f // 6 + f // 8, f - 3 - 2 * (f // 6) - f // 8

    group = lax.broadcasted_iota(jnp.int32, (near, LANES), 1) % rows

    def contract_third(f, mode):
        product = f >= 3
        left, right = pair_of(f)
        left = jnp.where(product, left, f)
        right = jnp.where(product, right, f)

        def piece(r, carry):
            value = fine[left, r] * jnp.where(product, fine[right, r], 1.0)
            value = value.reshape(blocks * near, fine_points)
            lines[r] = rows_times(value, third[r]).reshape(blocks, near, LANES)
            return carry

        lax.fori_loop(0, rows, piece, 0)
        masks = [group == flip(me_y, r) for r in range(rows)]
        _, tiles = spread(rows, mode)

        def regroup(q, carry):
            parts = [lines[r, q] for r in range(rows)]
            for j, side, u in tiles:
                out = parts[-1]
                for r in range(rows - 1):
                    out = jnp.where(masks[j ^ r], parts[r], out)
                if u == 0:
                    recv_a[f, side, q, own_lines(mode)] = out
                else:
                    send_a[f % slots_a, side, u - 1, q] = out
            return carry

        lax.fori_loop(0, blocks, regroup, 0)
        for side in (1, 0):
            for copy in copies_a(f, mode, side):
                copy.start()

    def free_a(f, mode):
        for side in (1, 0):
            for copy in copies_a(f, mode, side):
                copy.wait_send()

    def table_times(table, value):
        top, rest = split(value)
        both = dot(table, top)
        return both[:M] + both[M:] + dot(table[:M], rest)

    def partial_first(f, mode, side, h):
        value = jnp.concatenate([recv_a[f, side, 2 * h + i] for i in range(2)], axis=1)
        return table_times(first[mode], value)

    def first_out(f, mode):
        for copy in copies_a(f, mode, 1):
            copy.wait_recv()

        @pl.when(f >= slots_p)
        def _():
            copy_p(f - slots_p, mode).wait_send()

        def piece(h, carry):
            out = partial_first(f, mode, 1, h)
            for i in range(2):
                send_p[f % slots_p, 2 * h + i] = out[:, i * LANES : (i + 1) * LANES]
            return carry

        lax.fori_loop(0, blocks // 2, piece, 0)
        copy_p(f, mode).start()

    def first_in(f, mode):
        for copy in copies_a(f, mode, 0):
            copy.wait_recv()
        copy_p(f, mode).wait_recv()

        @pl.when(f >= slots_b)
        def _():
            for k in range(1, columns):
                copy_b(f - slots_b, k).wait_send()

        slot = f % slots_b

        def piece(h, carry):
            out = partial_first(f, mode, 0, h)
            for i in range(2):
                part = out[:, i * LANES : (i + 1) * LANES] + recv_p[f, 2 * h + i]
                send_b[slot, :, pl.ds(pl.multiple_of((2 * h + i) * rows, 8), rows)] = (
                    part.T.reshape(M // rows, rows, M)
                )
            return carry

        lax.fori_loop(0, blocks // 2, piece, 0)
        for k in range(1, columns):
            copy_b(f, k).start()
        recv_b[f, :, pl.ds(pl.multiple_of(me_z * depth, 8), depth)] = send_b[
            slot, pl.ds(me_z * share, share)
        ]

    def contract_second(f):
        for k in range(1, columns):
            copy_b(f, k).wait_recv()
        for h in range(share // 2):
            value = jnp.concatenate([recv_b[f, 2 * h + i] for i in range(2)], axis=1)
            out = table_times(second[...], value)
            for i in range(2):
                part = out[:, i * LANES : (i + 1) * LANES]
                for d in range(rows):
                    send_c[f, d, 2 * h + i] = part[d * band : (d + 1) * band]
        for j in range(1, rows):
            copy_c(f, j).start()
        recv_c[f, me_y] = send_c[f, me_y]

    def place(f, product):
        for j in range(1, rows):
            copy_c(f, j).wait_recv()
        whole = recv_c.at[f].reshape(rows * share * band, M)

        def line(m, carry):
            out = whole[pl.ds(m, block, stride=band), :]
            if product:
                left, right = pair_of(f)
                stress[f - 3, m] = out - filtered[left, m] * filtered[right, m]
            else:
                filtered[f, m] = out
            return carry

        lax.fori_loop(0, band, line, 0)

    def loop(start, stop, *work):
        def body(f, carry):
            for one in work:
                one(f)
            return carry

        lax.fori_loop(start, stop, body, 0)

    def loaded(c):
        pltpu.make_async_copy(fine.at[c], fine.at[c], load_sem.at[c]).wait()

    for copy in table_copies:
        copy.wait()

    for f in range(slots_a):
        if f < 3:
            loaded(f)
        contract_third(f, f % 2)

    points = base.shape[1]
    row = lax.broadcasted_iota(jnp.int32, (points, points), 0)
    column = lax.broadcasted_iota(jnp.int32, (points, points), 1)
    swap = jnp.where(row == flip_by(column, me_y, rows), 1.0, 0.0).astype(jnp.bfloat16)
    second[...] = dot(base[...], swap).astype(jnp.bfloat16)

    def steps(g):
        for mode in range(2):
            f = 2 * g + mode

            @pl.when(f < fields_count)
            def _():
                first_out(f, mode)

            @pl.when(f + slots_a < fields_count)
            def _():
                free_a(f, mode)
                contract_third(f + slots_a, mode)

            @pl.when((f >= 1) & (f <= fields_count))
            def _():
                first_in(f - 1, 1 - mode)

            @pl.when((f >= 2) & (f <= fields_count + 1))
            def _():
                contract_second(f - 2)

    loop(0, (fields_count + 3) // 2, steps)
    loop(0, 3, lambda f: place(f, False))
    loop(3, fields_count, lambda f: place(f, True))

    for f in range(fields_count - slots_a, fields_count):
        free_a(f, f % 2)
    for f in range(fields_count - slots_p, fields_count):
        copy_p(f, f % 2).wait_send()
    for f in range(fields_count - slots_b, fields_count):
        for k in range(1, columns):
            copy_b(f, k).wait_send()

    def finish(f):
        for j in range(1, rows):
            copy_c(f, j).wait_send()

    loop(0, fields_count, finish)


def tables(fine, rows, columns):
    matrix = line_filter(fine, M)
    block = M // columns
    share = block // rows
    near = fine // rows
    top, rest = halves(matrix)
    both = np.concatenate([top, rest])
    spot, group = np.arange(M) // rows, np.arange(M) % rows
    third = []
    for r in range(rows):
        order = spot // share * block + (group ^ r) * share + spot % share
        third.append(np.concatenate([top.T[:, order], rest.T[:, order]], axis=1))
    first = []
    for mode in range(2):
        step, _ = spread(rows, mode)
        spots = np.arange(rows // 2)
        for half in range(2):
            peers = spots // step * (2 * step) + half * step + spots % step
            order = (peers[:, None] * near + np.arange(near)).reshape(-1)
            first.append(both[:, order])
    return np.stack(third), np.stack(first).reshape(2, 2, 2 * M, fine // 2), both


def kernel_shards(velocity):
    rows, columns = lax.axis_size("py"), lax.axis_size("pz")
    _, near, depth, fine = velocity.shape
    blocks = depth // rows
    block, band = M // columns, M // rows
    share = block // rows
    half = rows // 2
    slots_a, slots_p, slots_b = 4, 2, 3
    third, first, base = tables(fine, rows, columns)
    vmem = pl.BlockSpec(memory_space=pltpu.VMEM)
    dma = pltpu.SemaphoreType.DMA
    f32 = jnp.float32
    return pl.pallas_call(
        functools.partial(kernel, rows, columns),
        out_shape=(
            jax.ShapeDtypeStruct((3, band, block, M), f32),
            jax.ShapeDtypeStruct((6, band, block, M), f32),
        ),
        in_specs=[pl.BlockSpec(memory_space=pl.ANY)] * 4,
        out_specs=(vmem, vmem),
        scratch_shapes=[
            pltpu.VMEM(third.shape, jnp.bfloat16),
            pltpu.VMEM(first.shape[1:], jnp.bfloat16),
            pltpu.VMEM(base.shape, jnp.bfloat16),
            pltpu.VMEM(base.shape, jnp.bfloat16),
            pltpu.VMEM((3, rows, blocks, near, fine), f32),
            pltpu.VMEM((rows, blocks, near, LANES), f32),
            pltpu.VMEM((slots_a, 2, half - 1, blocks, near, LANES), f32),
            pltpu.VMEM((fields_count, 2, blocks, half * near, LANES), f32),
            pltpu.VMEM((slots_p, blocks, M, LANES), f32),
            pltpu.VMEM((fields_count, blocks, M, LANES), f32),
            pltpu.VMEM((slots_b, columns * share, depth, M), f32),
            pltpu.VMEM((fields_count, share, columns * depth, M), f32),
            pltpu.VMEM((fields_count, rows, share, band, M), f32),
            pltpu.VMEM((fields_count, rows, share, band, M), f32),
            dma((4,)),
            dma((3,)),
            dma((fields_count, 2, half - 1)),
            dma((fields_count, 2, half - 1)),
            dma((fields_count,)),
            dma((fields_count,)),
            dma((fields_count, columns - 1)),
            dma((fields_count, columns - 1)),
            dma((fields_count, rows - 1)),
            dma((fields_count, rows - 1)),
        ],
        compiler_params=pltpu.CompilerParams(
            collective_id=0, has_side_effects=True, vmem_limit_bytes=67_000_000
        ),
    )(velocity, jnp.asarray(third), jnp.asarray(first), jnp.asarray(base))


def plain_shards(velocity):
    matrix = jnp.asarray(line_filter(velocity.shape[3], M))
    components = [velocity[component] for component in range(3)]
    fields = jnp.stack(components + [components[a] * components[b] for a, b in factor_pairs])
    high = lax.Precision.HIGHEST
    third = jnp.einsum("fabk,mk->fabm", fields, matrix, precision=high)
    third = lax.all_to_all(third, "pz", split_axis=3, concat_axis=2, tiled=True)
    second = jnp.einsum("fabm,nb->fanm", third, matrix, precision=high)
    second = lax.all_to_all(second, "py", split_axis=2, concat_axis=1, tiled=True)
    coarse = jnp.einsum("fanm,pa->fnmp", second, matrix, precision=high)
    stress = jnp.stack(
        [coarse[3 + p] - coarse[a] * coarse[b] for p, (a, b) in enumerate(factor_pairs)]
    )
    return coarse[:3], stress


def shards(velocity):
    rows, columns = lax.axis_size("py"), lax.axis_size("pz")
    _, lines, depth, fine = velocity.shape
    whole_tiles = (
        M == LANES
        and rows % 8 == 0
        and rows & (rows - 1) == 0
        and lines % 8 == 0
        and depth % (2 * rows) == 0
        and M % (2 * rows * columns) == 0
        and (M // rows) % 8 == 0
    )
    return kernel_shards(velocity) if whole_tiles else plain_shards(velocity)


def solution(mesh):
    placed = P(None, "py", "pz", None)
    return jax.shard_map(
        shards, mesh=mesh, in_specs=(placed,), out_specs=(placed, placed), check_vma=False
    )
```

```python
import functools
import math

import jax
import jax.numpy as jnp
import ml_dtypes
import numpy as np
from jax import lax
from jax.experimental import pallas as pl
from jax.experimental.pallas import tpu as pltpu
from jax.sharding import PartitionSpec as P

M = 128

factor_pairs = ((0, 0), (0, 1), (0, 2), (1, 1), (1, 2), (2, 2))
fields_count = 9
LANES = 128


def line_filter(fine, coarse):
    half = coarse // 2
    modes = np.arange(1, half)
    width = 2.0 * math.pi / coarse
    gain = np.exp(-(modes.astype(np.float64) ** 2) * (width * width / 24.0))
    turns = np.arange(coarse)[:, None] * fine - np.arange(fine)[None, :] * coarse
    period = fine * coarse
    matrix = np.ones((coarse, fine))
    for mode, weight in zip(modes, gain):
        matrix += 2.0 * weight * np.cos(2.0 * math.pi * ((mode * turns) % period) / period)
    return (matrix / fine).astype(np.float32)


def halves(matrix):
    top = matrix.astype(ml_dtypes.bfloat16)
    return top, (matrix - top.astype(np.float32)).astype(ml_dtypes.bfloat16)


def split(value):
    top = value.astype(jnp.bfloat16)
    return top, (value - top.astype(jnp.float32)).astype(jnp.bfloat16)


def dot(left, right):
    return jnp.dot(left, right, preferred_element_type=jnp.float32)


def rows_times(value, table):
    width = table.shape[1] // 2
    top, rest = split(value)
    both = dot(top, table)
    return both[:, :width] + both[:, width:] + dot(rest, table[:, :width])


def flip(me, bits):
    out, weight = me, 1
    while weight <= bits:
        if bits & weight:
            out = out + weight - 2 * weight * (me // weight % 2)
        weight *= 2
    return out


def flip_by(value, bits, rows):
    out, weight = value, 1
    while weight < rows:
        bit = bits // weight % 2
        out = out + bit * (weight - 2 * weight * (value // weight % 2))
        weight *= 2
    return out


def spread(rows, mode):
    step = rows // 2 if mode == 0 else rows // 4
    return step, [(j, j // step % 2, j // (2 * step) * step + j % step) for j in range(rows)]


def kernel(
    rows, columns, velocity, third_table, first_table, base_table, direct_third_table,
    direct_first_table, filtered, stress,
    third, first, base, second, direct_third, direct_first, fine, lines,
    send_a, recv_a, send_p, recv_p, send_b, recv_b, send_c, recv_c,
    natural, direct_lines, send_z, recv_z, send_y, recv_y, turned,
    table_sem, load_sem, natural_sem, send_a_sem, recv_a_sem, send_p_sem, recv_p_sem,
    send_b_sem, recv_b_sem, send_c_sem, recv_c_sem,
    send_z_sem, recv_z_sem, send_y_sem, recv_y_sem,
):
    me_y = lax.axis_index("py")
    me_z = lax.axis_index("pz")
    _, _, blocks, near, fine_points = fine.shape
    depth = rows * blocks
    block, band = M // columns, M // rows
    share = block // rows
    part = blocks // 2
    steps = near // columns
    spun = fields_count - 1
    slots_a, slots_p, slots_b = send_a.shape[0], send_p.shape[0], send_b.shape[0]
    MESH = pl.DeviceIdType.MESH

    strides = [spread(rows, mode)[0] for mode in range(2)]
    table_copies = [
        pltpu.make_async_copy(third_table, third, table_sem.at[0]),
        pltpu.make_async_copy(base_table, base, table_sem.at[1]),
        pltpu.make_async_copy(direct_third_table, direct_third, table_sem.at[2]),
        pltpu.make_async_copy(direct_first_table, direct_first, table_sem.at[3]),
    ] + [
        pltpu.make_async_copy(
            first_table.at[mode, me_y // strides[mode] % 2], first.at[mode], table_sem.at[4 + mode]
        )
        for mode in range(2)
    ]
    last_left, last_right = factor_pairs[-1]

    def load_natural(u):
        return pltpu.make_async_copy(
            velocity.at[last_left, pl.ds(u * 2 * columns, 2 * columns)],
            natural.at[u % 2],
            natural_sem.at[u],
        )

    def load(c):
        def line(b, carry):
            pltpu.make_async_copy(
                velocity.at[c, :, b, :], fine.at[c, b % rows, b // rows], load_sem.at[c]
            ).start()
            return carry

        lax.fori_loop(0, depth, line, 0)

    table_copies[0].start()
    load(0)
    for copy in table_copies[1:]:
        copy.start()
    for u in range(2):
        load_natural(u).start()
    load(1)
    load(2)

    barrier = pltpu.get_barrier_semaphore()
    for k in range(1, columns):
        pl.semaphore_signal(
            barrier, inc=1, device_id=(me_y, (me_z + k) % columns), device_id_type=MESH
        )
    for j in range(1, rows):
        pl.semaphore_signal(barrier, inc=1, device_id=(flip(me_y, j), me_z), device_id_type=MESH)
    pl.semaphore_wait(barrier, columns + rows - 2)

    def own_lines(mode):
        step = strides[mode]
        at = me_y // (2 * step) * step + me_y % step
        return pl.ds(pl.multiple_of(at * near, 8), near)

    def copies_a(f, mode, side):
        step, tiles = spread(rows, mode)
        return [
            pltpu.make_async_remote_copy(
                src_ref=send_a.at[f % slots_a, mode, side, u - 1],
                dst_ref=recv_a.at[f, mode, side, :, own_lines(mode)],
                send_sem=send_a_sem.at[f, mode, side, u - 1],
                recv_sem=recv_a_sem.at[f, mode, side, u - 1],
                device_id=(flip(me_y, j - side * step), me_z),
                device_id_type=MESH,
            )
            for j, s, u in tiles
            if s == side and u > 0
        ]

    def copy_p(f, mode):
        return pltpu.make_async_remote_copy(
            src_ref=send_p.at[f % slots_p, mode],
            dst_ref=recv_p.at[f, mode],
            send_sem=send_p_sem.at[f, mode],
            recv_sem=recv_p_sem.at[f, mode],
            device_id=(flip(me_y, strides[mode]), me_z),
            device_id_type=MESH,
        )

    def copy_b(f, mode, k):
        count = part * rows
        at = me_z * depth + mode * count
        return pltpu.make_async_remote_copy(
            src_ref=send_b.at[
                f % slots_b, pl.ds((me_z + k) % columns * share, share), pl.ds(mode * count, count)
            ],
            dst_ref=recv_b.at[f, :, pl.ds(pl.multiple_of(at, 8), count)],
            send_sem=send_b_sem.at[f, mode, k - 1],
            recv_sem=recv_b_sem.at[f, mode, k - 1],
            device_id=(me_y, (me_z + k) % columns),
            device_id_type=MESH,
        )

    def copy_c(f, j):
        return pltpu.make_async_remote_copy(
            src_ref=send_c.at[f, pl.ds(flip(me_y, j), 1)],
            dst_ref=recv_c.at[f, pl.ds(me_y, 1)],
            send_sem=send_c_sem.at[f, j - 1],
            recv_sem=recv_c_sem.at[f, j - 1],
            device_id=(flip(me_y, j), me_z),
            device_id_type=MESH,
        )

    def copy_z(u, k):
        return pltpu.make_async_remote_copy(
            src_ref=send_z.at[k - 1, pl.ds(2 * u, 2)],
            dst_ref=recv_z.at[pl.ds(2 * u, 2), pl.ds(pl.multiple_of(me_z * depth, 8), depth)],
            send_sem=send_z_sem.at[u, k - 1],
            recv_sem=recv_z_sem.at[u, k - 1],
            device_id=(me_y, (me_z + k) % columns),
            device_id_type=MESH,
        )

    def copy_y(j):
        return pltpu.make_async_remote_copy(
            src_ref=send_y.at[flip(me_y, j)],
            dst_ref=recv_y.at[pl.ds(me_y * steps, steps)],
            send_sem=send_y_sem.at[j - 1],
            recv_sem=recv_y_sem.at[j - 1],
            device_id=(flip(me_y, j), me_z),
            device_id_type=MESH,
        )

    def pair_of(f):
        return f // 6 + f // 8, f - 3 - 2 * (f // 6) - f // 8

    def contract_third(f):
        product = f >= 3
        left, right = pair_of(f)
        left = jnp.where(product, left, f)
        right = jnp.where(product, right, f)
        group = lax.broadcasted_iota(jnp.int32, (near, LANES), 1) % rows
        masks = [group == flip(me_y, r) for r in range(rows)]
        for mode in range(2):
            _, tiles = spread(rows, mode)
            where = pl.ds(mode * part, part)

            def piece(r, carry):
                value = fine[left, r, where] * jnp.where(product, fine[right, r, where], 1.0)
                value = value.reshape(part * near, fine_points)
                lines[r] = rows_times(value, third[r]).reshape(part, near, LANES)
                return carry

            lax.fori_loop(0, rows, piece, 0)

            def regroup(q, carry):
                parts = [lines[r, q] for r in range(rows)]
                for j, side, u in tiles:
                    out = parts[-1]
                    for r in range(rows - 1):
                        out = jnp.where(masks[j ^ r], parts[r], out)
                    if u == 0:
                        recv_a[f, mode, side, q, own_lines(mode)] = out
                    else:
                        send_a[f % slots_a, mode, side, u - 1, q] = out
                return carry

            lax.fori_loop(0, part, regroup, 0)
            for side in (1, 0):
                for copy in copies_a(f, mode, side):
                    copy.start()

    def free_a(f):
        for mode in range(2):
            for side in (1, 0):
                for copy in copies_a(f, mode, side):
                    copy.wait_send()

    def table_times(table, value):
        top, rest = split(value)
        both = dot(table, top)
        return both[:M] + both[M:] + dot(table[:M], rest)

    def partial_first(f, mode, side):
        for at in range(0, part, 2):
            spots = range(at, min(at + 2, part))
            value = jnp.concatenate([recv_a[f, mode, side, q] for q in spots], axis=1)
            out = table_times(first[mode], value)
            for i, q in enumerate(spots):
                yield q, out[:, i * LANES : (i + 1) * LANES]

    def first_out(f):
        for mode in range(2):
            for copy in copies_a(f, mode, 1):
                copy.wait_recv()

            @pl.when(f >= slots_p)
            def _():
                copy_p(f - slots_p, mode).wait_send()

            for q, out in partial_first(f, mode, 1):
                send_p[f % slots_p, mode, q] = out
            copy_p(f, mode).start()

    def first_in(f):
        slot = f % slots_b
        for mode in range(2):
            for copy in copies_a(f, mode, 0):
                copy.wait_recv()
            copy_p(f, mode).wait_recv()

            @pl.when(f >= slots_b)
            def _():
                for k in range(1, columns):
                    copy_b(f - slots_b, mode, k).wait_send()

            count = part * rows
            for q, out in partial_first(f, mode, 0):
                out = out + recv_p[f, mode, q]
                send_b[slot, :, pl.ds(mode * count + q * rows, rows)] = out.T.reshape(
                    M // rows, rows, M
                )
            for k in range(1, columns):
                copy_b(f, mode, k).start()
            at = pl.multiple_of(me_z * depth + mode * count, 8)
            recv_b[f, :, pl.ds(at, count)] = send_b[
                slot, pl.ds(me_z * share, share), pl.ds(mode * count, count)
            ]

    def contract_second(f):
        for mode in range(2):
            for k in range(1, columns):
                copy_b(f, mode, k).wait_recv()
        for h in range(share // 2):
            value = jnp.concatenate([recv_b[f, 2 * h + i] for i in range(2)], axis=1)
            out = table_times(second[...], value)
            for i in range(2):
                piece = out[:, i * LANES : (i + 1) * LANES]
                for d in range(rows):
                    send_c[f, d, 2 * h + i] = piece[d * band : (d + 1) * band]
        for j in range(1, rows):
            copy_c(f, j).start()
        recv_c[f, me_y] = send_c[f, me_y]

    def place(f, product):
        for j in range(1, rows):
            copy_c(f, j).wait_recv()
        whole = recv_c.at[f].reshape(rows * share * band, M)

        def line(m, carry):
            out = whole[pl.ds(m, block, stride=band), :]
            if product:
                left, right = pair_of(f)
                stress[f - 3, m] = out - filtered[left, m] * filtered[right, m]
            else:
                filtered[f, m] = out
            return carry

        lax.fori_loop(0, band, line, 0)

    def direct_contract_third():
        group = lax.broadcasted_iota(jnp.int32, (depth, LANES), 1) // block
        masks = [group == (me_z + k) % columns for k in range(columns)]
        units = steps // 2

        def unit(u, carry):
            load_natural(u).wait()

            def piece(s, inner):
                value = jnp.concatenate(
                    [natural[u % 2, i * columns + s] for i in range(2)], axis=0
                )
                value = value * value
                direct_lines[s] = rows_times(value, direct_third[s]).reshape(2, depth, LANES)
                return inner

            lax.fori_loop(0, columns, piece, 0)

            @pl.when(u + 2 < units)
            def _():
                load_natural(u + 2).start()

            for i in range(2):
                parts = [direct_lines[s, i] for s in range(columns)]
                for k in range(columns):
                    out = parts[-1]
                    for s in range(columns - 1):
                        out = jnp.where(masks[(k + s) % columns], parts[s], out)
                    if k == 0:
                        recv_z[2 * u + i, pl.ds(pl.multiple_of(me_z * depth, 8), depth)] = out
                    else:
                        send_z[k - 1, 2 * u + i] = out
            for k in range(1, columns):
                copy_z(u, k).start()
            return carry

        lax.fori_loop(0, units, unit, 0)

    def direct_contract_second():
        def piece(h, carry):
            for k in range(1, columns):
                copy_z(h, k).wait_recv()
            value = jnp.concatenate([recv_z[2 * h + i] for i in range(2)], axis=1)
            out = table_times(base[...], value)
            for i in range(2):
                for d in range(rows):
                    send_y[d, 2 * h + i] = out[
                        d * band : (d + 1) * band, i * LANES : (i + 1) * LANES
                    ]
            return carry

        lax.fori_loop(0, steps // 2, piece, 0)
        for j in range(1, rows):
            copy_y(j).start()
        recv_y[pl.ds(me_y * steps, steps)] = send_y[me_y]

    def direct_contract_first():
        for j in range(1, rows):
            copy_y(j).wait_recv()
        pad = jnp.zeros((LANES - rows * steps, LANES), jnp.float32)
        for m in range(band):
            plane = jnp.concatenate([recv_y[:, m, :], pad], axis=0).T
            for g in range(columns):
                turned[g, m * block : (m + 1) * block] = plane[g * block : (g + 1) * block]
        out = jnp.zeros((band * block, M), jnp.float32)
        for g in range(columns):
            table = direct_first[(g + columns - me_z) % columns]
            out = out + rows_times(turned[g], table)
        out = out.reshape(band, block, M)
        stress[spun - 3] = out - filtered[last_left] * filtered[last_right]

    def loop(start, stop, *work):
        def body(f, carry):
            for one in work:
                one(f)
            return carry

        lax.fori_loop(start, stop, body, 0)

    def loaded(c):
        pltpu.make_async_copy(fine.at[c], fine.at[c], load_sem.at[c]).wait()

    table_copies[0].wait()
    loaded(0)
    contract_third(0)
    for copy in table_copies[1:]:
        copy.wait()
    direct_contract_third()
    loaded(1)
    contract_third(1)
    loaded(2)

    points = base.shape[1]
    row = lax.broadcasted_iota(jnp.int32, (points, points), 0)
    column = lax.broadcasted_iota(jnp.int32, (points, points), 1)
    swap = jnp.where(row == flip_by(column, me_y, rows), 1.0, 0.0).astype(jnp.bfloat16)
    second[...] = dot(base[...], swap).astype(jnp.bfloat16)

    def round_of(f):
        first_out(f)

        @pl.when(f + slots_a < spun)
        def _():
            free_a(f)
            contract_third(f + slots_a)

        @pl.when(f >= 1)
        def _():
            first_in(f - 1)

    loop(0, spun - 1, round_of)
    first_out(spun - 1)
    loop(0, spun - 3, contract_second)
    direct_contract_second()
    first_in(spun - 2)
    contract_second(spun - 3)
    first_in(spun - 1)
    loop(0, 3, lambda f: place(f, False))
    contract_second(spun - 2)
    loop(3, spun - 3, lambda f: place(f, True))
    direct_contract_first()
    contract_second(spun - 1)
    loop(spun - 3, spun, lambda f: place(f, True))

    loop(spun - slots_a, spun, free_a)

    def drain_p(f):
        for mode in range(2):
            copy_p(f, mode).wait_send()

    loop(spun - slots_p, spun, drain_p)

    def drain_b(f):
        for mode in range(2):
            for k in range(1, columns):
                copy_b(f, mode, k).wait_send()

    loop(spun - slots_b, spun, drain_b)

    def drain_c(f):
        for j in range(1, rows):
            copy_c(f, j).wait_send()

    loop(0, spun, drain_c)

    def drain_z(u):
        for k in range(1, columns):
            copy_z(u, k).wait_send()

    loop(0, steps // 2, drain_z)
    for j in range(1, rows):
        copy_y(j).wait_send()


def tables(fine, rows, columns):
    matrix = line_filter(fine, M)
    block = M // columns
    share = block // rows
    near = fine // rows
    steps = near // columns
    top, rest = halves(matrix)
    both = np.concatenate([top, rest])
    spot, group = np.arange(M) // rows, np.arange(M) % rows
    third = []
    for r in range(rows):
        order = spot // share * block + (group ^ r) * share + spot % share
        third.append(np.concatenate([top.T[:, order], rest.T[:, order]], axis=1))
    first = []
    for mode in range(2):
        step, _ = spread(rows, mode)
        spots = np.arange(rows // 2)
        for half in range(2):
            peers = spots // step * (2 * step) + half * step + spots % step
            order = (peers[:, None] * near + np.arange(near)).reshape(-1)
            first.append(both[:, order])
    first = np.stack(first).reshape(2, 2, 2 * M, fine // 2)
    direct_third, direct_first = [], []
    for s in range(columns):
        order = np.concatenate(
            [np.arange(block) + (g - s) % columns * block for g in range(columns)]
        )
        direct_third.append(np.concatenate([top.T[:, order], rest.T[:, order]], axis=1))
        points = np.arange(rows * steps) * columns + s
        table = np.concatenate([top.T[points], rest.T[points]], axis=1)
        direct_first.append(np.pad(table, ((0, LANES - rows * steps), (0, 0))))
    return np.stack(third), first, both, np.stack(direct_third), np.stack(direct_first)


def kernel_shards(velocity):
    rows, columns = lax.axis_size("py"), lax.axis_size("pz")
    _, near, depth, fine = velocity.shape
    blocks = depth // rows
    block, band = M // columns, M // rows
    share = block // rows
    half, part, steps = rows // 2, blocks // 2, near // columns
    spun = fields_count - 1
    slots_a, slots_p, slots_b = 2, 2, 2
    constants = tables(fine, rows, columns)
    third, first, base, direct_third, direct_first = constants
    vmem = pl.BlockSpec(memory_space=pltpu.VMEM)
    dma = pltpu.SemaphoreType.DMA
    f32, bf16 = jnp.float32, jnp.bfloat16
    return pl.pallas_call(
        functools.partial(kernel, rows, columns),
        out_shape=(
            jax.ShapeDtypeStruct((3, band, block, M), f32),
            jax.ShapeDtypeStruct((6, band, block, M), f32),
        ),
        in_specs=[pl.BlockSpec(memory_space=pl.ANY)] * (1 + len(constants)),
        out_specs=(vmem, vmem),
        scratch_shapes=[
            pltpu.VMEM(third.shape, bf16),
            pltpu.VMEM(first.shape[1:], bf16),
            pltpu.VMEM(base.shape, bf16),
            pltpu.VMEM(base.shape, bf16),
            pltpu.VMEM(direct_third.shape, bf16),
            pltpu.VMEM(direct_first.shape, bf16),
            pltpu.VMEM((3, rows, blocks, near, fine), f32),
            pltpu.VMEM((rows, part, near, LANES), f32),
            pltpu.VMEM((slots_a, 2, 2, half - 1, part, near, LANES), f32),
            pltpu.VMEM((spun, 2, 2, part, half * near, LANES), f32),
            pltpu.VMEM((slots_p, 2, part, M, LANES), f32),
            pltpu.VMEM((spun, 2, part, M, LANES), f32),
            pltpu.VMEM((slots_b, columns * share, depth, M), f32),
            pltpu.VMEM((spun, share, columns * depth, M), f32),
            pltpu.VMEM((spun, rows, share, band, M), f32),
            pltpu.VMEM((spun, rows, share, band, M), f32),
            pltpu.VMEM((2, 2 * columns, depth, fine), f32),
            pltpu.VMEM((columns, 2, depth, LANES), f32),
            pltpu.VMEM((columns - 1, steps, depth, LANES), f32),
            pltpu.VMEM((steps, columns * depth, LANES), f32),
            pltpu.VMEM((rows, steps, band, LANES), f32),
            pltpu.VMEM((rows * steps, band, LANES), f32),
            pltpu.VMEM((columns, band * block, LANES), f32),
            dma((6,)),
            dma((3,)),
            dma((steps // 2,)),
            dma((spun, 2, 2, half - 1)),
            dma((spun, 2, 2, half - 1)),
            dma((spun, 2)),
            dma((spun, 2)),
            dma((spun, 2, columns - 1)),
            dma((spun, 2, columns - 1)),
            dma((spun, rows - 1)),
            dma((spun, rows - 1)),
            dma((steps // 2, columns - 1)),
            dma((steps // 2, columns - 1)),
            dma((rows - 1,)),
            dma((rows - 1,)),
        ],
        compiler_params=pltpu.CompilerParams(
            collective_id=0, has_side_effects=True, vmem_limit_bytes=67_000_000
        ),
    )(velocity, *[jnp.asarray(constant) for constant in constants])


def plain_shards(velocity):
    matrix = jnp.asarray(line_filter(velocity.shape[3], M))
    components = [velocity[component] for component in range(3)]
    fields = jnp.stack(components + [components[a] * components[b] for a, b in factor_pairs])
    high = lax.Precision.HIGHEST
    third = jnp.einsum("fabk,mk->fabm", fields, matrix, precision=high)
    third = lax.all_to_all(third, "pz", split_axis=3, concat_axis=2, tiled=True)
    second = jnp.einsum("fabm,nb->fanm", third, matrix, precision=high)
    second = lax.all_to_all(second, "py", split_axis=2, concat_axis=1, tiled=True)
    coarse = jnp.einsum("fanm,pa->fnmp", second, matrix, precision=high)
    stress = jnp.stack(
        [coarse[3 + p] - coarse[a] * coarse[b] for p, (a, b) in enumerate(factor_pairs)]
    )
    return coarse[:3], stress


def shards(velocity):
    rows, columns = lax.axis_size("py"), lax.axis_size("pz")
    _, lines, depth, fine = velocity.shape
    whole_tiles = (
        M == LANES
        and rows % 8 == 0
        and rows & (rows - 1) == 0
        and lines % 8 == 0
        and lines % (2 * columns) == 0
        and depth % (2 * rows) == 0
        and M % (2 * rows * columns) == 0
        and (M // rows) % 8 == 0
        and rows * (lines // columns) <= LANES
    )
    return kernel_shards(velocity) if whole_tiles else plain_shards(velocity)


def solution(mesh):
    placed = P(None, "py", "pz", None)
    return jax.shard_map(
        shards, mesh=mesh, in_specs=(placed,), out_specs=(placed, placed), check_vma=False
    )
```

```python
import functools
import math

import jax
import jax.numpy as jnp
import ml_dtypes
import numpy as np
from jax import lax
from jax.experimental import pallas as pl
from jax.experimental.pallas import tpu as pltpu
from jax.sharding import PartitionSpec as P

M = 128

factor_pairs = ((0, 0), (0, 1), (0, 2), (1, 1), (1, 2), (2, 2))
fields_count = 9
LANES = 128


def line_filter(fine, coarse):
    half = coarse // 2
    modes = np.arange(1, half)
    width = 2.0 * math.pi / coarse
    gain = np.exp(-(modes.astype(np.float64) ** 2) * (width * width / 24.0))
    turns = np.arange(coarse)[:, None] * fine - np.arange(fine)[None, :] * coarse
    period = fine * coarse
    matrix = np.ones((coarse, fine))
    for mode, weight in zip(modes, gain):
        matrix += 2.0 * weight * np.cos(2.0 * math.pi * ((mode * turns) % period) / period)
    return (matrix / fine).astype(np.float32)


def halves(matrix):
    top = matrix.astype(ml_dtypes.bfloat16)
    return top, (matrix - top.astype(np.float32)).astype(ml_dtypes.bfloat16)


def split(value):
    top = value.astype(jnp.bfloat16)
    return top, (value - top.astype(jnp.float32)).astype(jnp.bfloat16)


def dot(left, right):
    return jnp.dot(left, right, preferred_element_type=jnp.float32)


def rows_times(value, table):
    width = table.shape[1] // 2
    top, rest = split(value)
    both = dot(top, table)
    return both[:, :width] + both[:, width:] + dot(rest, table[:, :width])


def flip(me, bits):
    out, weight = me, 1
    while weight <= bits:
        if bits & weight:
            out = out + weight - 2 * weight * (me // weight % 2)
        weight *= 2
    return out


def flip_by(value, bits, rows):
    out, weight = value, 1
    while weight < rows:
        bit = bits // weight % 2
        out = out + bit * (weight - 2 * weight * (value // weight % 2))
        weight *= 2
    return out


def spread(rows, mode):
    step = rows // 2 if mode == 0 else rows // 4
    return step, [(j, j // step % 2, j // (2 * step) * step + j % step) for j in range(rows)]


def kernel(
    rows, columns, velocity, third_table, first_table, base_table, direct_third_table,
    direct_first_table, filtered_out, stress_out,
    filtered, stress, third, first, base, second, direct_third, direct_first, fine, lines,
    send_a, recv_a, send_p, recv_p, send_b, recv_b, send_c, recv_c,
    natural, direct_lines, send_z, recv_z, send_y, recv_y, turned,
    out_sem, table_sem, load_sem, natural_sem, send_a_sem, recv_a_sem, send_p_sem, recv_p_sem,
    send_b_sem, recv_b_sem, send_c_sem, recv_c_sem,
    send_z_sem, recv_z_sem, send_y_sem, recv_y_sem,
):
    me_y = lax.axis_index("py")
    me_z = lax.axis_index("pz")
    _, _, blocks, near, fine_points = fine.shape
    depth = rows * blocks
    block, band = M // columns, M // rows
    share = block // rows
    part = blocks // 2
    steps = near // columns
    spun = fields_count - 1
    slots_a, slots_p, slots_b = send_a.shape[0], send_p.shape[0], send_b.shape[0]
    MESH = pl.DeviceIdType.MESH

    strides = [spread(rows, mode)[0] for mode in range(2)]
    table_copies = [
        pltpu.make_async_copy(third_table, third, table_sem.at[0]),
        pltpu.make_async_copy(base_table, base, table_sem.at[1]),
        pltpu.make_async_copy(direct_third_table, direct_third, table_sem.at[2]),
        pltpu.make_async_copy(direct_first_table, direct_first, table_sem.at[3]),
    ] + [
        pltpu.make_async_copy(
            first_table.at[mode, me_y // strides[mode] % 2], first.at[mode], table_sem.at[4]
        )
        for mode in range(2)
    ]
    last_left, last_right = factor_pairs[-1]

    def settle(ref, sem):
        pltpu.make_async_copy(ref, ref, sem).wait()

    def load_natural(u):
        return pltpu.make_async_copy(
            velocity.at[last_left, pl.ds(u * 2 * columns, 2 * columns)],
            natural.at[u % 2],
            natural_sem.at[u % 2],
        )

    def load(c):
        def lines_of(r, carry):
            for q in range(blocks):
                pltpu.make_async_copy(
                    velocity.at[c, :, q * rows + r, :], fine.at[c, r, q], load_sem.at[r]
                ).start()
            return carry

        lax.fori_loop(0, rows, lines_of, 0)

    def loaded(c, r):
        settle(fine.at[c, r], load_sem.at[r])

    barrier = pltpu.get_barrier_semaphore()
    for k in range(1, columns):
        pl.semaphore_signal(
            barrier, inc=1, device_id=(me_y, (me_z + k) % columns), device_id_type=MESH
        )
    for j in range(1, rows):
        pl.semaphore_signal(barrier, inc=1, device_id=(flip(me_y, j), me_z), device_id_type=MESH)

    table_copies[0].start()
    load(0)

    def own_lines(mode):
        step = strides[mode]
        at = me_y // (2 * step) * step + me_y % step
        return pl.ds(pl.multiple_of(at * near, 8), near)

    def copies_a(f, mode, side):
        step, tiles = spread(rows, mode)
        return [
            pltpu.make_async_remote_copy(
                src_ref=send_a.at[f % slots_a, mode, side, u - 1],
                dst_ref=recv_a.at[f, mode, side, :, own_lines(mode)],
                send_sem=send_a_sem.at[f % slots_a],
                recv_sem=recv_a_sem.at[f, mode, side],
                device_id=(flip(me_y, j - side * step), me_z),
                device_id_type=MESH,
            )
            for j, s, u in tiles
            if s == side and u > 0
        ]

    def copy_p(f, mode):
        return pltpu.make_async_remote_copy(
            src_ref=send_p.at[f % slots_p, mode],
            dst_ref=recv_p.at[f, mode],
            send_sem=send_p_sem.at[f % slots_p, mode],
            recv_sem=recv_p_sem.at[f, mode],
            device_id=(flip(me_y, strides[mode]), me_z),
            device_id_type=MESH,
        )

    def copy_b(f, mode, k):
        count = part * rows
        at = me_z * depth + mode * count
        return pltpu.make_async_remote_copy(
            src_ref=send_b.at[
                f % slots_b, pl.ds((me_z + k) % columns * share, share), pl.ds(mode * count, count)
            ],
            dst_ref=recv_b.at[f, :, pl.ds(pl.multiple_of(at, 8), count)],
            send_sem=send_b_sem.at[f % slots_b, mode],
            recv_sem=recv_b_sem.at[f],
            device_id=(me_y, (me_z + k) % columns),
            device_id_type=MESH,
        )

    def free_b(f, mode):
        count = part * rows
        sent = send_b.at[
            f % slots_b, pl.ds(0, (columns - 1) * share), pl.ds(mode * count, count)
        ]
        settle(sent, send_b_sem.at[f % slots_b, mode])

    def copy_c(f, j):
        return pltpu.make_async_remote_copy(
            src_ref=send_c.at[f, pl.ds(flip(me_y, j), 1)],
            dst_ref=recv_c.at[f, pl.ds(me_y, 1)],
            send_sem=send_c_sem.at[0],
            recv_sem=recv_c_sem.at[f],
            device_id=(flip(me_y, j), me_z),
            device_id_type=MESH,
        )

    def copy_z(u, k):
        return pltpu.make_async_remote_copy(
            src_ref=send_z.at[k - 1, pl.ds(2 * u, 2)],
            dst_ref=recv_z.at[pl.ds(2 * u, 2), pl.ds(pl.multiple_of(me_z * depth, 8), depth)],
            send_sem=send_z_sem.at[0],
            recv_sem=recv_z_sem.at[u],
            device_id=(me_y, (me_z + k) % columns),
            device_id_type=MESH,
        )

    def copy_y(j):
        return pltpu.make_async_remote_copy(
            src_ref=send_y.at[flip(me_y, j)],
            dst_ref=recv_y.at[pl.ds(me_y * steps, steps)],
            send_sem=send_y_sem.at[0],
            recv_sem=recv_y_sem.at[0],
            device_id=(flip(me_y, j), me_z),
            device_id_type=MESH,
        )

    def pair_of(f):
        return f // 6 + f // 8, f - 3 - 2 * (f // 6) - f // 8

    def contract_third(f):
        product = f >= 3
        left, right = pair_of(f)
        left = jnp.where(product, left, f)
        right = jnp.where(product, right, f)
        group = lax.broadcasted_iota(jnp.int32, (near, LANES), 1) % rows
        masks = [group == flip(me_y, r) for r in range(rows)]

        def piece(r, carry):
            @pl.when(f < 3)
            def _():
                loaded(f, r)

            value = fine[left, r] * jnp.where(product, fine[right, r], 1.0)
            value = value.reshape(blocks * near, fine_points)
            lines[r] = rows_times(value, third[r]).reshape(blocks, near, LANES)
            return carry

        lax.fori_loop(0, rows, piece, 0)
        for mode in range(2):
            _, tiles = spread(rows, mode)

            def regroup(q, carry):
                parts = [lines[r, mode * part + q] for r in range(rows)]
                for j, side, u in tiles:
                    out = parts[-1]
                    for r in range(rows - 1):
                        out = jnp.where(masks[j ^ r], parts[r], out)
                    if u == 0:
                        recv_a[f, mode, side, q, own_lines(mode)] = out
                    else:
                        send_a[f % slots_a, mode, side, u - 1, q] = out
                return carry

            lax.fori_loop(0, part, regroup, 0)
            if mode == 0:

                @pl.when(f == 0)
                def _():
                    pl.semaphore_wait(barrier, columns + rows - 2)

            for side in (1, 0):
                for copy in copies_a(f, mode, side):
                    copy.start()

    def free_a(f):
        settle(send_a.at[f % slots_a], send_a_sem.at[f % slots_a])

    def arrived_a(f, mode, side):
        others = (rows // 2 - 1) * near
        settle(recv_a.at[f, mode, side, :, pl.ds(0, others)], recv_a_sem.at[f, mode, side])

    def table_times(table, value):
        top, rest = split(value)
        both = dot(table, top)
        return both[:M] + both[M:] + dot(table[:M], rest)

    def partial_first(f, mode, side):
        for at in range(0, part, 2):
            spots = range(at, min(at + 2, part))
            value = jnp.concatenate([recv_a[f, mode, side, q] for q in spots], axis=1)
            out = table_times(first[mode], value)
            for i, q in enumerate(spots):
                yield q, out[:, i * LANES : (i + 1) * LANES]

    def first_out(f):
        for mode in range(2):
            arrived_a(f, mode, 1)

            @pl.when(f >= slots_p)
            def _():
                copy_p(f - slots_p, mode).wait_send()

            for q, out in partial_first(f, mode, 1):
                send_p[f % slots_p, mode, q] = out
            copy_p(f, mode).start()

    def first_in(f):
        slot = f % slots_b
        for mode in range(2):
            arrived_a(f, mode, 0)
            copy_p(f, mode).wait_recv()

            @pl.when(f >= slots_b)
            def _():
                free_b(f - slots_b, mode)

            count = part * rows
            for q, out in partial_first(f, mode, 0):
                out = out + recv_p[f, mode, q]
                send_b[slot, :, pl.ds(mode * count + q * rows, rows)] = out.T.reshape(
                    M // rows, rows, M
                )
            for k in range(1, columns):
                copy_b(f, mode, k).start()
            at = pl.multiple_of(me_z * depth + mode * count, 8)
            recv_b[f, :, pl.ds(at, count)] = send_b[
                slot, pl.ds(me_z * share, share), pl.ds(mode * count, count)
            ]

    def contract_second(f):
        settle(recv_b.at[f, :, pl.ds(0, (columns - 1) * depth)], recv_b_sem.at[f])
        for h in range(share // 2):
            value = jnp.concatenate([recv_b[f, 2 * h + i] for i in range(2)], axis=1)
            out = table_times(second[...], value)
            for i in range(2):
                piece = out[:, i * LANES : (i + 1) * LANES]
                for d in range(rows):
                    send_c[f, d, 2 * h + i] = piece[d * band : (d + 1) * band]
        for j in range(1, rows):
            copy_c(f, j).start()
        recv_c[f, me_y] = send_c[f, me_y]

    def store(f, product):
        source, target, at = (stress, stress_out, f - 3) if product else (filtered, filtered_out, f)
        return pltpu.make_async_copy(source.at[at], target.at[at], out_sem.at[int(product)])

    def place(f, product):
        settle(recv_c.at[f, pl.ds(0, rows - 1)], recv_c_sem.at[f])
        whole = recv_c.at[f].reshape(rows * share * band, M)

        def line(m, carry):
            out = whole[pl.ds(m, block, stride=band), :]
            if product:
                left, right = pair_of(f)
                stress[f - 3, m] = out - filtered[left, m] * filtered[right, m]
            else:
                filtered[f, m] = out
            return carry

        lax.fori_loop(0, band, line, 0)
        store(f, product).start()

    def direct_contract_third():
        group = lax.broadcasted_iota(jnp.int32, (depth, LANES), 1) // block
        masks = [group == (me_z + k) % columns for k in range(columns)]
        units = steps // 2

        def unit(u, carry):
            load_natural(u).wait()

            def piece(s, inner):
                value = jnp.concatenate(
                    [natural[u % 2, i * columns + s] for i in range(2)], axis=0
                )
                value = value * value
                direct_lines[s] = rows_times(value, direct_third[s]).reshape(2, depth, LANES)
                return inner

            lax.fori_loop(0, columns, piece, 0)

            @pl.when(u + 2 < units)
            def _():
                load_natural(u + 2).start()

            for i in range(2):
                parts = [direct_lines[s, i] for s in range(columns)]
                for k in range(columns):
                    out = parts[-1]
                    for s in range(columns - 1):
                        out = jnp.where(masks[(k + s) % columns], parts[s], out)
                    if k == 0:
                        recv_z[2 * u + i, pl.ds(pl.multiple_of(me_z * depth, 8), depth)] = out
                    else:
                        send_z[k - 1, 2 * u + i] = out
            for k in range(1, columns):
                copy_z(u, k).start()
            return carry

        lax.fori_loop(0, units, unit, 0)

    def direct_contract_second():
        def piece(h, carry):
            others = pl.ds(0, (columns - 1) * depth)
            settle(recv_z.at[pl.ds(2 * h, 2), others], recv_z_sem.at[h])
            value = jnp.concatenate([recv_z[2 * h + i] for i in range(2)], axis=1)
            out = table_times(base[...], value)
            for i in range(2):
                for d in range(rows):
                    send_y[d, 2 * h + i] = out[
                        d * band : (d + 1) * band, i * LANES : (i + 1) * LANES
                    ]
            return carry

        lax.fori_loop(0, steps // 2, piece, 0)
        for j in range(1, rows):
            copy_y(j).start()
        recv_y[pl.ds(me_y * steps, steps)] = send_y[me_y]

    def direct_contract_first():
        settle(recv_y.at[pl.ds(0, (rows - 1) * steps)], recv_y_sem.at[0])
        pad = jnp.zeros((LANES - rows * steps, LANES), jnp.float32)
        for m in range(band):
            plane = jnp.concatenate([recv_y[:, m, :], pad], axis=0).T
            for g in range(columns):
                turned[g, m * block : (m + 1) * block] = plane[g * block : (g + 1) * block]
        out = jnp.zeros((band * block, M), jnp.float32)
        for g in range(columns):
            table = direct_first[(g + columns - me_z) % columns]
            out = out + rows_times(turned[g], table)
        out = out.reshape(band, block, M)
        stress[spun - 3] = out - filtered[last_left] * filtered[last_right]
        store(spun, True).start()

    def loop(start, stop, *work):
        def body(f, carry):
            for one in work:
                one(f)
            return carry

        lax.fori_loop(start, stop, body, 0)

    table_copies[0].wait()

    def opening(f):
        contract_third(f)
        load(f + 1)

        @pl.when(f == 0)
        def _():
            for copy in table_copies[1:]:
                copy.start()
            for u in range(2):
                load_natural(u).start()

    loop(0, slots_a, opening)
    for copy in table_copies[1:4]:
        copy.wait()
    settle(first, table_sem.at[4])
    direct_contract_third()

    points = base.shape[1]
    row = lax.broadcasted_iota(jnp.int32, (points, points), 0)
    column = lax.broadcasted_iota(jnp.int32, (points, points), 1)
    swap = jnp.where(row == flip_by(column, me_y, rows), 1.0, 0.0).astype(jnp.bfloat16)
    second[...] = dot(base[...], swap).astype(jnp.bfloat16)

    def round_of(f):
        first_out(f)

        @pl.when(f + slots_a < spun)
        def _():
            free_a(f)
            contract_third(f + slots_a)

        @pl.when(f >= 1)
        def _():
            first_in(f - 1)

    loop(0, spun - 1, round_of)
    first_out(spun - 1)
    loop(0, spun - 3, contract_second)
    direct_contract_second()
    first_in(spun - 2)
    contract_second(spun - 3)
    first_in(spun - 1)
    loop(0, 3, lambda f: place(f, False))
    contract_second(spun - 2)
    loop(3, spun - 3, lambda f: place(f, True))
    direct_contract_first()
    contract_second(spun - 1)
    loop(spun - 3, spun, lambda f: place(f, True))

    loop(spun - slots_a, spun, free_a)

    def drain_p(f):
        for mode in range(2):
            copy_p(f, mode).wait_send()

    loop(spun - slots_p, spun, drain_p)

    def drain_b(f):
        for mode in range(2):
            free_b(f, mode)

    loop(spun - slots_b, spun, drain_b)

    settle(send_c.at[:, pl.ds(0, rows - 1)], send_c_sem.at[0])
    settle(send_z, send_z_sem.at[0])
    settle(send_y.at[pl.ds(0, rows - 1)], send_y_sem.at[0])
    settle(filtered, out_sem.at[0])
    settle(stress, out_sem.at[1])


def tables(fine, rows, columns):
    matrix = line_filter(fine, M)
    block = M // columns
    share = block // rows
    near = fine // rows
    steps = near // columns
    top, rest = halves(matrix)
    both = np.concatenate([top, rest])
    spot, group = np.arange(M) // rows, np.arange(M) % rows
    third = []
    for r in range(rows):
        order = spot // share * block + (group ^ r) * share + spot % share
        third.append(np.concatenate([top.T[:, order], rest.T[:, order]], axis=1))
    first = []
    for mode in range(2):
        step, _ = spread(rows, mode)
        spots = np.arange(rows // 2)
        for half in range(2):
            peers = spots // step * (2 * step) + half * step + spots % step
            order = (peers[:, None] * near + np.arange(near)).reshape(-1)
            first.append(both[:, order])
    first = np.stack(first).reshape(2, 2, 2 * M, fine // 2)
    direct_third, direct_first = [], []
    for s in range(columns):
        order = np.concatenate(
            [np.arange(block) + (g - s) % columns * block for g in range(columns)]
        )
        direct_third.append(np.concatenate([top.T[:, order], rest.T[:, order]], axis=1))
        points = np.arange(rows * steps) * columns + s
        table = np.concatenate([top.T[points], rest.T[points]], axis=1)
        direct_first.append(np.pad(table, ((0, LANES - rows * steps), (0, 0))))
    return np.stack(third), first, both, np.stack(direct_third), np.stack(direct_first)


def kernel_shards(velocity):
    rows, columns = lax.axis_size("py"), lax.axis_size("pz")
    _, near, depth, fine = velocity.shape
    blocks = depth // rows
    block, band = M // columns, M // rows
    share = block // rows
    half, part, steps = rows // 2, blocks // 2, near // columns
    spun = fields_count - 1
    slots_a, slots_p, slots_b = 2, 2, 2
    constants = tables(fine, rows, columns)
    third, first, base, direct_third, direct_first = constants
    dma = pltpu.SemaphoreType.DMA
    f32, bf16 = jnp.float32, jnp.bfloat16
    return pl.pallas_call(
        functools.partial(kernel, rows, columns),
        out_shape=(
            jax.ShapeDtypeStruct((3, band, block, M), f32),
            jax.ShapeDtypeStruct((6, band, block, M), f32),
        ),
        in_specs=[pl.BlockSpec(memory_space=pl.ANY)] * (1 + len(constants)),
        out_specs=(pl.BlockSpec(memory_space=pl.ANY),) * 2,
        scratch_shapes=[
            pltpu.VMEM((3, band, block, M), f32),
            pltpu.VMEM((6, band, block, M), f32),
            pltpu.VMEM(third.shape, bf16),
            pltpu.VMEM(first.shape[1:], bf16),
            pltpu.VMEM(base.shape, bf16),
            pltpu.VMEM(base.shape, bf16),
            pltpu.VMEM(direct_third.shape, bf16),
            pltpu.VMEM(direct_first.shape, bf16),
            pltpu.VMEM((3, rows, blocks, near, fine), f32),
            pltpu.VMEM((rows, blocks, near, LANES), f32),
            pltpu.VMEM((slots_a, 2, 2, half - 1, part, near, LANES), f32),
            pltpu.VMEM((spun, 2, 2, part, half * near, LANES), f32),
            pltpu.VMEM((slots_p, 2, part, M, LANES), f32),
            pltpu.VMEM((spun, 2, part, M, LANES), f32),
            pltpu.VMEM((slots_b, columns * share, depth, M), f32),
            pltpu.VMEM((spun, share, columns * depth, M), f32),
            pltpu.VMEM((spun, rows, share, band, M), f32),
            pltpu.VMEM((spun, rows, share, band, M), f32),
            pltpu.VMEM((2, 2 * columns, depth, fine), f32),
            pltpu.VMEM((columns, 2, depth, LANES), f32),
            pltpu.VMEM((columns - 1, steps, depth, LANES), f32),
            pltpu.VMEM((steps, columns * depth, LANES), f32),
            pltpu.VMEM((rows, steps, band, LANES), f32),
            pltpu.VMEM((rows * steps, band, LANES), f32),
            pltpu.VMEM((columns, band * block, LANES), f32),
            dma((2,)),
            dma((5,)),
            dma((rows,)),
            dma((2,)),
            dma((slots_a,)),
            dma((spun, 2, 2)),
            dma((slots_p, 2)),
            dma((spun, 2)),
            dma((slots_b, 2)),
            dma((spun,)),
            dma((1,)),
            dma((spun,)),
            dma((1,)),
            dma((steps // 2,)),
            dma((1,)),
            dma((1,)),
        ],
        compiler_params=pltpu.CompilerParams(
            collective_id=0, has_side_effects=True, vmem_limit_bytes=67_000_000
        ),
    )(velocity, *[jnp.asarray(constant) for constant in constants])


def plain_shards(velocity):
    matrix = jnp.asarray(line_filter(velocity.shape[3], M))
    components = [velocity[component] for component in range(3)]
    fields = jnp.stack(components + [components[a] * components[b] for a, b in factor_pairs])
    high = lax.Precision.HIGHEST
    third = jnp.einsum("fabk,mk->fabm", fields, matrix, precision=high)
    third = lax.all_to_all(third, "pz", split_axis=3, concat_axis=2, tiled=True)
    second = jnp.einsum("fabm,nb->fanm", third, matrix, precision=high)
    second = lax.all_to_all(second, "py", split_axis=2, concat_axis=1, tiled=True)
    coarse = jnp.einsum("fanm,pa->fnmp", second, matrix, precision=high)
    stress = jnp.stack(
        [coarse[3 + p] - coarse[a] * coarse[b] for p, (a, b) in enumerate(factor_pairs)]
    )
    return coarse[:3], stress


def shards(velocity):
    rows, columns = lax.axis_size("py"), lax.axis_size("pz")
    _, lines, depth, fine = velocity.shape
    whole_tiles = (
        M == LANES
        and rows % 8 == 0
        and rows & (rows - 1) == 0
        and lines % 8 == 0
        and lines % (2 * columns) == 0
        and depth % (2 * rows) == 0
        and M % (2 * rows * columns) == 0
        and (M // rows) % 8 == 0
        and rows * (lines // columns) <= LANES
    )
    return kernel_shards(velocity) if whole_tiles else plain_shards(velocity)


def solution(mesh):
    placed = P(None, "py", "pz", None)
    return jax.shard_map(
        shards, mesh=mesh, in_specs=(placed,), out_specs=(placed, placed), check_vma=False
    )
```

```python
import functools
import math

import jax
import jax.numpy as jnp
import ml_dtypes
import numpy as np
from jax import lax
from jax.experimental import pallas as pl
from jax.experimental.pallas import tpu as pltpu
from jax.sharding import PartitionSpec as P

M = 128

factor_pairs = ((0, 0), (0, 1), (0, 2), (1, 1), (1, 2), (2, 2))
fields_count = 9
LANES = 128


def line_filter(fine, coarse):
    half = coarse // 2
    modes = np.arange(1, half)
    width = 2.0 * math.pi / coarse
    gain = np.exp(-(modes.astype(np.float64) ** 2) * (width * width / 24.0))
    turns = np.arange(coarse)[:, None] * fine - np.arange(fine)[None, :] * coarse
    period = fine * coarse
    matrix = np.ones((coarse, fine))
    for mode, weight in zip(modes, gain):
        matrix += 2.0 * weight * np.cos(2.0 * math.pi * ((mode * turns) % period) / period)
    return (matrix / fine).astype(np.float32)


def halves(matrix):
    top = matrix.astype(ml_dtypes.bfloat16)
    return top, (matrix - top.astype(np.float32)).astype(ml_dtypes.bfloat16)


def split(value):
    top = value.astype(jnp.bfloat16)
    return top, (value - top.astype(jnp.float32)).astype(jnp.bfloat16)


def dot(left, right):
    return jnp.dot(left, right, preferred_element_type=jnp.float32)


def rows_times(value, table):
    width = table.shape[1] // 2
    top, rest = split(value)
    both = dot(top, table)
    return both[:, :width] + both[:, width:] + dot(rest, table[:, :width])


def flip(me, bits):
    out, weight = me, 1
    while weight <= bits:
        if bits & weight:
            out = out + weight - 2 * weight * (me // weight % 2)
        weight *= 2
    return out


def flip_by(value, bits, rows):
    out, weight = value, 1
    while weight < rows:
        bit = bits // weight % 2
        out = out + bit * (weight - 2 * weight * (value // weight % 2))
        weight *= 2
    return out


def spread(rows, mode):
    step = rows // 2 if mode == 0 else rows // 4
    return step, [(j, j // step % 2, j // (2 * step) * step + j % step) for j in range(rows)]


def kernel(
    rows, columns, velocity, third_table, first_table, base_table, direct_third_table,
    direct_first_table, filtered_out, stress_out,
    filtered, stress, third, first, base, second, direct_third, direct_first, fine, lines,
    send_a, recv_a, send_p, recv_p, send_b, recv_b, send_c, recv_c,
    natural, direct_lines, send_z, recv_z, send_y, recv_y, turned,
    out_sem, table_sem, load_sem, natural_sem, send_a_sem, recv_a_sem, send_p_sem, recv_p_sem,
    send_b_sem, recv_b_sem, send_c_sem, recv_c_sem,
    send_z_sem, recv_z_sem, send_y_sem, recv_y_sem,
):
    me_y = lax.axis_index("py")
    me_z = lax.axis_index("pz")
    _, _, blocks, near, fine_points = fine.shape
    depth = rows * blocks
    block, band = M // columns, M // rows
    share = block // rows
    part = blocks // 2
    steps = near // columns
    spun = fields_count - 1
    slots_a, slots_p, slots_b = send_a.shape[0], send_p.shape[0], send_b.shape[0]
    MESH = pl.DeviceIdType.MESH

    strides = [spread(rows, mode)[0] for mode in range(2)]
    table_copies = [
        pltpu.make_async_copy(third_table, third, table_sem.at[0]),
        pltpu.make_async_copy(base_table, base, table_sem.at[1]),
        pltpu.make_async_copy(direct_third_table, direct_third, table_sem.at[2]),
        pltpu.make_async_copy(direct_first_table, direct_first, table_sem.at[3]),
    ] + [
        pltpu.make_async_copy(
            first_table.at[mode, me_y // strides[mode] % 2], first.at[mode], table_sem.at[4]
        )
        for mode in range(2)
    ]
    last_left, last_right = factor_pairs[-1]

    def settle(ref, sem):
        pltpu.make_async_copy(ref, ref, sem).wait()

    def load_natural(u):
        return pltpu.make_async_copy(
            velocity.at[last_left, pl.ds(u * 2 * columns, 2 * columns)],
            natural.at[u % 2],
            natural_sem.at[u % 2],
        )

    def load(c):
        def lines_of(r, carry):
            for q in range(blocks):
                pltpu.make_async_copy(
                    velocity.at[c, :, q * rows + r, :], fine.at[c, r, q], load_sem.at[r]
                ).start()
            return carry

        lax.fori_loop(0, rows, lines_of, 0)

    def loaded(c, r):
        settle(fine.at[c, r], load_sem.at[r])

    barrier = pltpu.get_barrier_semaphore()
    for k in range(1, columns):
        pl.semaphore_signal(
            barrier, inc=1, device_id=(me_y, (me_z + k) % columns), device_id_type=MESH
        )
    for j in range(1, rows):
        pl.semaphore_signal(barrier, inc=1, device_id=(flip(me_y, j), me_z), device_id_type=MESH)

    table_copies[0].start()
    load(0)
    for u in range(2):
        load_natural(u).start()
    for copy in table_copies[1:]:
        copy.start()

    def own_lines(mode):
        step = strides[mode]
        at = me_y // (2 * step) * step + me_y % step
        return pl.ds(pl.multiple_of(at * near, 8), near)

    def copies_a(f, mode, side):
        step, tiles = spread(rows, mode)
        return [
            pltpu.make_async_remote_copy(
                src_ref=send_a.at[f % slots_a, mode, side, u - 1],
                dst_ref=recv_a.at[f, mode, side, :, own_lines(mode)],
                send_sem=send_a_sem.at[f % slots_a],
                recv_sem=recv_a_sem.at[f, mode, side],
                device_id=(flip(me_y, j - side * step), me_z),
                device_id_type=MESH,
            )
            for j, s, u in tiles
            if s == side and u > 0
        ]

    def copy_p(f, mode):
        return pltpu.make_async_remote_copy(
            src_ref=send_p.at[f % slots_p, mode],
            dst_ref=recv_p.at[f, mode],
            send_sem=send_p_sem.at[f % slots_p, mode],
            recv_sem=recv_p_sem.at[f, mode],
            device_id=(flip(me_y, strides[mode]), me_z),
            device_id_type=MESH,
        )

    def copy_b(f, mode, k):
        count = part * rows
        at = me_z * depth + mode * count
        return pltpu.make_async_remote_copy(
            src_ref=send_b.at[
                f % slots_b, pl.ds((me_z + k) % columns * share, share), pl.ds(mode * count, count)
            ],
            dst_ref=recv_b.at[f, :, pl.ds(pl.multiple_of(at, 8), count)],
            send_sem=send_b_sem.at[f % slots_b, mode],
            recv_sem=recv_b_sem.at[f],
            device_id=(me_y, (me_z + k) % columns),
            device_id_type=MESH,
        )

    def free_b(f, mode):
        count = part * rows
        sent = send_b.at[
            f % slots_b, pl.ds(0, (columns - 1) * share), pl.ds(mode * count, count)
        ]
        settle(sent, send_b_sem.at[f % slots_b, mode])

    def copy_c(f, j):
        return pltpu.make_async_remote_copy(
            src_ref=send_c.at[f, pl.ds(flip(me_y, j), 1)],
            dst_ref=recv_c.at[f, pl.ds(me_y, 1)],
            send_sem=send_c_sem.at[0],
            recv_sem=recv_c_sem.at[f],
            device_id=(flip(me_y, j), me_z),
            device_id_type=MESH,
        )

    def copy_z(u, k):
        return pltpu.make_async_remote_copy(
            src_ref=send_z.at[k - 1, pl.ds(2 * u, 2)],
            dst_ref=recv_z.at[pl.ds(2 * u, 2), pl.ds(pl.multiple_of(me_z * depth, 8), depth)],
            send_sem=send_z_sem.at[0],
            recv_sem=recv_z_sem.at[u],
            device_id=(me_y, (me_z + k) % columns),
            device_id_type=MESH,
        )

    def copy_y(j):
        return pltpu.make_async_remote_copy(
            src_ref=send_y.at[flip(me_y, j)],
            dst_ref=recv_y.at[pl.ds(me_y * steps, steps)],
            send_sem=send_y_sem.at[0],
            recv_sem=recv_y_sem.at[0],
            device_id=(flip(me_y, j), me_z),
            device_id_type=MESH,
        )

    def pair_of(f):
        return f // 6 + f // 8, f - 3 - 2 * (f // 6) - f // 8

    def contract_third(f):
        product = f >= 3
        left, right = pair_of(f)
        left = jnp.where(product, left, f)
        right = jnp.where(product, right, f)
        group = lax.broadcasted_iota(jnp.int32, (near, LANES), 1) % rows
        masks = [group == flip(me_y, r) for r in range(rows)]

        def piece(r, carry):
            @pl.when(f < 3)
            def _():
                loaded(f, r)

            value = fine[left, r] * jnp.where(product, fine[right, r], 1.0)
            value = value.reshape(blocks * near, fine_points)
            lines[r] = rows_times(value, third[r]).reshape(blocks, near, LANES)
            return carry

        lax.fori_loop(0, rows, piece, 0)
        for mode in range(2):
            _, tiles = spread(rows, mode)

            def regroup(q, carry):
                parts = [lines[r, mode * part + q] for r in range(rows)]
                for j, side, u in tiles:
                    out = parts[-1]
                    for r in range(rows - 1):
                        out = jnp.where(masks[j ^ r], parts[r], out)
                    if u == 0:
                        recv_a[f, mode, side, q, own_lines(mode)] = out
                    else:
                        send_a[f % slots_a, mode, side, u - 1, q] = out
                return carry

            lax.fori_loop(0, part, regroup, 0)
            if mode == 0:

                @pl.when(f == 0)
                def _():
                    pl.semaphore_wait(barrier, columns + rows - 2)

            for side in (1, 0):
                for copy in copies_a(f, mode, side):
                    copy.start()

    def free_a(f):
        settle(send_a.at[f % slots_a], send_a_sem.at[f % slots_a])

    def arrived_a(f, mode, side):
        others = (rows // 2 - 1) * near
        settle(recv_a.at[f, mode, side, :, pl.ds(0, others)], recv_a_sem.at[f, mode, side])

    def table_times(table, value):
        top, rest = split(value)
        both = dot(table, top)
        return both[:M] + both[M:] + dot(table[:M], rest)

    def partial_first(f, mode, side):
        for at in range(0, part, 2):
            spots = range(at, min(at + 2, part))
            value = jnp.concatenate([recv_a[f, mode, side, q] for q in spots], axis=1)
            out = table_times(first[mode], value)
            for i, q in enumerate(spots):
                yield q, out[:, i * LANES : (i + 1) * LANES]

    def first_out(f):
        for mode in range(2):
            arrived_a(f, mode, 1)

            @pl.when(f >= slots_p)
            def _():
                copy_p(f - slots_p, mode).wait_send()

            for q, out in partial_first(f, mode, 1):
                send_p[f % slots_p, mode, q] = out
            copy_p(f, mode).start()

    def first_in(f):
        slot = f % slots_b
        for mode in range(2):
            arrived_a(f, mode, 0)
            copy_p(f, mode).wait_recv()

            @pl.when(f >= slots_b)
            def _():
                free_b(f - slots_b, mode)

            count = part * rows
            for q, out in partial_first(f, mode, 0):
                out = out + recv_p[f, mode, q]
                send_b[slot, :, pl.ds(mode * count + q * rows, rows)] = out.T.reshape(
                    M // rows, rows, M
                )
            for k in range(1, columns):
                copy_b(f, mode, k).start()
            at = pl.multiple_of(me_z * depth + mode * count, 8)
            recv_b[f, :, pl.ds(at, count)] = send_b[
                slot, pl.ds(me_z * share, share), pl.ds(mode * count, count)
            ]

    def contract_second(f):
        settle(recv_b.at[f, :, pl.ds(0, (columns - 1) * depth)], recv_b_sem.at[f])
        for h in range(share // 2):
            value = jnp.concatenate([recv_b[f, 2 * h + i] for i in range(2)], axis=1)
            out = table_times(second[...], value)
            for i in range(2):
                piece = out[:, i * LANES : (i + 1) * LANES]
                for d in range(rows):
                    send_c[f, d, 2 * h + i] = piece[d * band : (d + 1) * band]
        for j in range(1, rows):
            copy_c(f, j).start()
        recv_c[f, me_y] = send_c[f, me_y]

    def store(f, product):
        source, target, at = (stress, stress_out, f - 3) if product else (filtered, filtered_out, f)
        return pltpu.make_async_copy(source.at[at], target.at[at], out_sem.at[int(product)])

    def place(f, product):
        settle(recv_c.at[f, pl.ds(0, rows - 1)], recv_c_sem.at[f])
        whole = recv_c.at[f].reshape(rows * share * band, M)

        def line(m, carry):
            out = whole[pl.ds(m, block, stride=band), :]
            if product:
                left, right = pair_of(f)
                stress[f - 3, m] = out - filtered[left, m] * filtered[right, m]
            else:
                filtered[f, m] = out
            return carry

        lax.fori_loop(0, band, line, 0)
        store(f, product).start()

    def direct_contract_third(begin, end):
        group = lax.broadcasted_iota(jnp.int32, (depth, LANES), 1) // block
        masks = [group == (me_z + k) % columns for k in range(columns)]
        units = steps // 2

        def unit(u, carry):
            load_natural(u).wait()

            def piece(s, inner):
                value = jnp.concatenate(
                    [natural[u % 2, i * columns + s] for i in range(2)], axis=0
                )
                value = value * value
                direct_lines[s] = rows_times(value, direct_third[s]).reshape(2, depth, LANES)
                return inner

            lax.fori_loop(0, columns, piece, 0)

            @pl.when(u + 2 < units)
            def _():
                load_natural(u + 2).start()

            for i in range(2):
                parts = [direct_lines[s, i] for s in range(columns)]
                for k in range(columns):
                    out = parts[-1]
                    for s in range(columns - 1):
                        out = jnp.where(masks[(k + s) % columns], parts[s], out)
                    if k == 0:
                        recv_z[2 * u + i, pl.ds(pl.multiple_of(me_z * depth, 8), depth)] = out
                    else:
                        send_z[k - 1, 2 * u + i] = out
            for k in range(1, columns):
                copy_z(u, k).start()
            return carry

        lax.fori_loop(begin, end, unit, 0)

    def direct_contract_second():
        def piece(h, carry):
            others = pl.ds(0, (columns - 1) * depth)
            settle(recv_z.at[pl.ds(2 * h, 2), others], recv_z_sem.at[h])
            value = jnp.concatenate([recv_z[2 * h + i] for i in range(2)], axis=1)
            out = table_times(base[...], value)
            for i in range(2):
                for d in range(rows):
                    send_y[d, 2 * h + i] = out[
                        d * band : (d + 1) * band, i * LANES : (i + 1) * LANES
                    ]
            return carry

        lax.fori_loop(0, steps // 2, piece, 0)
        for j in range(1, rows):
            copy_y(j).start()
        recv_y[pl.ds(me_y * steps, steps)] = send_y[me_y]

    def direct_contract_first():
        settle(recv_y.at[pl.ds(0, (rows - 1) * steps)], recv_y_sem.at[0])
        pad = jnp.zeros((LANES - rows * steps, LANES), jnp.float32)
        for m in range(band):
            plane = jnp.concatenate([recv_y[:, m, :], pad], axis=0).T
            for g in range(columns):
                turned[g, m * block : (m + 1) * block] = plane[g * block : (g + 1) * block]
        out = jnp.zeros((band * block, M), jnp.float32)
        for g in range(columns):
            table = direct_first[(g + columns - me_z) % columns]
            out = out + rows_times(turned[g], table)
        out = out.reshape(band, block, M)
        stress[spun - 3] = out - filtered[last_left] * filtered[last_right]
        store(spun, True).start()

    def loop(start, stop, *work):
        def body(f, carry):
            for one in work:
                one(f)
            return carry

        lax.fori_loop(start, stop, body, 0)

    table_copies[0].wait()

    def opening(f):
        contract_third(f)

        @pl.when(f == 0)
        def _():
            for copy in table_copies[1:4]:
                copy.wait()
            settle(first, table_sem.at[4])

        load(f + 1)
        direct_contract_third(f, 1 + f * (steps // 2 - 1))

    loop(0, slots_a, opening)

    points = base.shape[1]
    row = lax.broadcasted_iota(jnp.int32, (points, points), 0)
    column = lax.broadcasted_iota(jnp.int32, (points, points), 1)
    swap = jnp.where(row == flip_by(column, me_y, rows), 1.0, 0.0).astype(jnp.bfloat16)
    second[...] = dot(base[...], swap).astype(jnp.bfloat16)

    def round_of(f):
        first_out(f)

        @pl.when(f + slots_a < spun)
        def _():
            free_a(f)
            contract_third(f + slots_a)

        @pl.when(f >= 1)
        def _():
            first_in(f - 1)

    loop(0, spun - 1, round_of)
    first_out(spun - 1)
    loop(0, spun - 3, contract_second)
    direct_contract_second()
    first_in(spun - 2)
    contract_second(spun - 3)
    first_in(spun - 1)
    loop(0, 3, lambda f: place(f, False))
    contract_second(spun - 2)
    loop(3, spun - 3, lambda f: place(f, True))
    direct_contract_first()
    contract_second(spun - 1)
    loop(spun - 3, spun, lambda f: place(f, True))

    loop(spun - slots_a, spun, free_a)

    def drain_p(f):
        for mode in range(2):
            copy_p(f, mode).wait_send()

    loop(spun - slots_p, spun, drain_p)

    def drain_b(f):
        for mode in range(2):
            free_b(f, mode)

    loop(spun - slots_b, spun, drain_b)

    settle(send_c.at[:, pl.ds(0, rows - 1)], send_c_sem.at[0])
    settle(send_z, send_z_sem.at[0])
    settle(send_y.at[pl.ds(0, rows - 1)], send_y_sem.at[0])
    settle(filtered, out_sem.at[0])
    settle(stress, out_sem.at[1])


def tables(fine, rows, columns):
    matrix = line_filter(fine, M)
    block = M // columns
    share = block // rows
    near = fine // rows
    steps = near // columns
    top, rest = halves(matrix)
    both = np.concatenate([top, rest])
    spot, group = np.arange(M) // rows, np.arange(M) % rows
    third = []
    for r in range(rows):
        order = spot // share * block + (group ^ r) * share + spot % share
        third.append(np.concatenate([top.T[:, order], rest.T[:, order]], axis=1))
    first = []
    for mode in range(2):
        step, _ = spread(rows, mode)
        spots = np.arange(rows // 2)
        for half in range(2):
            peers = spots // step * (2 * step) + half * step + spots % step
            order = (peers[:, None] * near + np.arange(near)).reshape(-1)
            first.append(both[:, order])
    first = np.stack(first).reshape(2, 2, 2 * M, fine // 2)
    direct_third, direct_first = [], []
    for s in range(columns):
        order = np.concatenate(
            [np.arange(block) + (g - s) % columns * block for g in range(columns)]
        )
        direct_third.append(np.concatenate([top.T[:, order], rest.T[:, order]], axis=1))
        points = np.arange(rows * steps) * columns + s
        table = np.concatenate([top.T[points], rest.T[points]], axis=1)
        direct_first.append(np.pad(table, ((0, LANES - rows * steps), (0, 0))))
    return np.stack(third), first, both, np.stack(direct_third), np.stack(direct_first)


def kernel_shards(velocity):
    rows, columns = lax.axis_size("py"), lax.axis_size("pz")
    _, near, depth, fine = velocity.shape
    blocks = depth // rows
    block, band = M // columns, M // rows
    share = block // rows
    half, part, steps = rows // 2, blocks // 2, near // columns
    spun = fields_count - 1
    slots_a, slots_p, slots_b = 2, 2, 2
    constants = tables(fine, rows, columns)
    third, first, base, direct_third, direct_first = constants
    dma = pltpu.SemaphoreType.DMA
    f32, bf16 = jnp.float32, jnp.bfloat16
    return pl.pallas_call(
        functools.partial(kernel, rows, columns),
        out_shape=(
            jax.ShapeDtypeStruct((3, band, block, M), f32),
            jax.ShapeDtypeStruct((6, band, block, M), f32),
        ),
        in_specs=[pl.BlockSpec(memory_space=pl.ANY)] * (1 + len(constants)),
        out_specs=(pl.BlockSpec(memory_space=pl.ANY),) * 2,
        scratch_shapes=[
            pltpu.VMEM((3, band, block, M), f32),
            pltpu.VMEM((6, band, block, M), f32),
            pltpu.VMEM(third.shape, bf16),
            pltpu.VMEM(first.shape[1:], bf16),
            pltpu.VMEM(base.shape, bf16),
            pltpu.VMEM(base.shape, bf16),
            pltpu.VMEM(direct_third.shape, bf16),
            pltpu.VMEM(direct_first.shape, bf16),
            pltpu.VMEM((3, rows, blocks, near, fine), f32),
            pltpu.VMEM((rows, blocks, near, LANES), f32),
            pltpu.VMEM((slots_a, 2, 2, half - 1, part, near, LANES), f32),
            pltpu.VMEM((spun, 2, 2, part, half * near, LANES), f32),
            pltpu.VMEM((slots_p, 2, part, M, LANES), f32),
            pltpu.VMEM((spun, 2, part, M, LANES), f32),
            pltpu.VMEM((slots_b, columns * share, depth, M), f32),
            pltpu.VMEM((spun, share, columns * depth, M), f32),
            pltpu.VMEM((spun, rows, share, band, M), f32),
            pltpu.VMEM((spun, rows, share, band, M), f32),
            pltpu.VMEM((2, 2 * columns, depth, fine), f32),
            pltpu.VMEM((columns, 2, depth, LANES), f32),
            pltpu.VMEM((columns - 1, steps, depth, LANES), f32),
            pltpu.VMEM((steps, columns * depth, LANES), f32),
            pltpu.VMEM((rows, steps, band, LANES), f32),
            pltpu.VMEM((rows * steps, band, LANES), f32),
            pltpu.VMEM((columns, band * block, LANES), f32),
            dma((2,)),
            dma((5,)),
            dma((rows,)),
            dma((2,)),
            dma((slots_a,)),
            dma((spun, 2, 2)),
            dma((slots_p, 2)),
            dma((spun, 2)),
            dma((slots_b, 2)),
            dma((spun,)),
            dma((1,)),
            dma((spun,)),
            dma((1,)),
            dma((steps // 2,)),
            dma((1,)),
            dma((1,)),
        ],
        compiler_params=pltpu.CompilerParams(
            collective_id=0, has_side_effects=True, vmem_limit_bytes=67_000_000
        ),
    )(velocity, *[jnp.asarray(constant) for constant in constants])


def plain_shards(velocity):
    matrix = jnp.asarray(line_filter(velocity.shape[3], M))
    components = [velocity[component] for component in range(3)]
    fields = jnp.stack(components + [components[a] * components[b] for a, b in factor_pairs])
    high = lax.Precision.HIGHEST
    third = jnp.einsum("fabk,mk->fabm", fields, matrix, precision=high)
    third = lax.all_to_all(third, "pz", split_axis=3, concat_axis=2, tiled=True)
    second = jnp.einsum("fabm,nb->fanm", third, matrix, precision=high)
    second = lax.all_to_all(second, "py", split_axis=2, concat_axis=1, tiled=True)
    coarse = jnp.einsum("fanm,pa->fnmp", second, matrix, precision=high)
    stress = jnp.stack(
        [coarse[3 + p] - coarse[a] * coarse[b] for p, (a, b) in enumerate(factor_pairs)]
    )
    return coarse[:3], stress


def shards(velocity):
    rows, columns = lax.axis_size("py"), lax.axis_size("pz")
    _, lines, depth, fine = velocity.shape
    whole_tiles = (
        M == LANES
        and rows % 8 == 0
        and rows & (rows - 1) == 0
        and lines % 8 == 0
        and lines % (2 * columns) == 0
        and depth % (2 * rows) == 0
        and M % (2 * rows * columns) == 0
        and (M // rows) % 8 == 0
        and rows * (lines // columns) <= LANES
    )
    return kernel_shards(velocity) if whole_tiles else plain_shards(velocity)


def solution(mesh):
    placed = P(None, "py", "pz", None)
    return jax.shard_map(
        shards, mesh=mesh, in_specs=(placed,), out_specs=(placed, placed), check_vma=False
    )
```

```python
import functools
import math

import jax
import jax.numpy as jnp
import ml_dtypes
import numpy as np
from jax import lax
from jax.experimental import pallas as pl
from jax.experimental.pallas import tpu as pltpu
from jax.sharding import PartitionSpec as P

M = 128

factor_pairs = ((0, 0), (0, 1), (0, 2), (1, 1), (1, 2), (2, 2))
fields_count = 9
LANES = 128


def line_filter(fine, coarse):
    half = coarse // 2
    modes = np.arange(1, half)
    width = 2.0 * math.pi / coarse
    gain = np.exp(-(modes.astype(np.float64) ** 2) * (width * width / 24.0))
    turns = np.arange(coarse)[:, None] * fine - np.arange(fine)[None, :] * coarse
    period = fine * coarse
    matrix = np.ones((coarse, fine))
    for mode, weight in zip(modes, gain):
        matrix += 2.0 * weight * np.cos(2.0 * math.pi * ((mode * turns) % period) / period)
    return (matrix / fine).astype(np.float32)


def halves(matrix):
    top = matrix.astype(ml_dtypes.bfloat16)
    return top, (matrix - top.astype(np.float32)).astype(ml_dtypes.bfloat16)


def split(value):
    top = value.astype(jnp.bfloat16)
    return top, (value - top.astype(jnp.float32)).astype(jnp.bfloat16)


def dot(left, right):
    return jnp.dot(left, right, preferred_element_type=jnp.float32)


def rows_times(value, table):
    width = table.shape[1] // 2
    top, rest = split(value)
    both = dot(top, table)
    return both[:, :width] + both[:, width:] + dot(rest, table[:, :width])


def flip(me, bits):
    out, weight = me, 1
    while weight <= bits:
        if bits & weight:
            out = out + weight - 2 * weight * (me // weight % 2)
        weight *= 2
    return out


def flip_by(value, bits, rows):
    out, weight = value, 1
    while weight < rows:
        bit = bits // weight % 2
        out = out + bit * (weight - 2 * weight * (value // weight % 2))
        weight *= 2
    return out


def spread(rows, mode):
    step = rows // 2 if mode == 0 else rows // 4
    return step, [(j, j // step % 2, j // (2 * step) * step + j % step) for j in range(rows)]


def kernel(
    rows, columns, velocity, third_table, first_table, base_table, direct_third_table,
    direct_first_table, filtered_out, stress_out,
    filtered, stress, third, first, base, second, direct_third, direct_first, fine, lines,
    send_a, recv_a, send_p, recv_p, send_b, recv_b, send_c, recv_c,
    natural, direct_lines, send_z, recv_z, send_y, recv_y, turned,
    out_sem, table_sem, load_sem, natural_sem, send_a_sem, recv_a_sem, send_p_sem, recv_p_sem,
    send_b_sem, recv_b_sem, send_c_sem, recv_c_sem,
    send_z_sem, recv_z_sem, send_y_sem, recv_y_sem,
):
    me_y = lax.axis_index("py")
    me_z = lax.axis_index("pz")
    _, _, blocks, near, fine_points = fine.shape
    depth = rows * blocks
    block, band = M // columns, M // rows
    share = block // rows
    part = blocks // 2
    steps = near // columns
    spun = fields_count - 1
    slots_a, slots_p, slots_b = send_a.shape[0], send_p.shape[0], send_b.shape[0]
    MESH = pl.DeviceIdType.MESH

    strides = [spread(rows, mode)[0] for mode in range(2)]
    table_copies = [
        pltpu.make_async_copy(third_table, third, table_sem.at[0]),
        pltpu.make_async_copy(base_table, base, table_sem.at[1]),
        pltpu.make_async_copy(direct_third_table, direct_third, table_sem.at[2]),
        pltpu.make_async_copy(direct_first_table, direct_first, table_sem.at[3]),
    ] + [
        pltpu.make_async_copy(
            first_table.at[mode, me_y // strides[mode] % 2], first.at[mode], table_sem.at[4]
        )
        for mode in range(2)
    ]
    last_left, last_right = factor_pairs[-1]

    def settle(ref, sem):
        pltpu.make_async_copy(ref, ref, sem).wait()

    def load_natural(u):
        return pltpu.make_async_copy(
            velocity.at[last_left, pl.ds(u * 2 * columns, 2 * columns)],
            natural.at[u % 2],
            natural_sem.at[u % 2],
        )

    def load(c):
        def lines_of(r, carry):
            for q in range(blocks):
                pltpu.make_async_copy(
                    velocity.at[c, :, q * rows + r, :], fine.at[c, r, q], load_sem.at[r]
                ).start()
            return carry

        lax.fori_loop(0, rows, lines_of, 0)

    def loaded(c, r):
        settle(fine.at[c, r], load_sem.at[r])

    barrier = pltpu.get_barrier_semaphore()
    for k in range(1, columns):
        pl.semaphore_signal(
            barrier, inc=1, device_id=(me_y, (me_z + k) % columns), device_id_type=MESH
        )
    for j in range(1, rows):
        pl.semaphore_signal(barrier, inc=1, device_id=(flip(me_y, j), me_z), device_id_type=MESH)

    table_copies[0].start()
    load(0)
    for u in range(2):
        load_natural(u).start()
    for copy in table_copies[1:]:
        copy.start()

    def own_lines(mode):
        step = strides[mode]
        at = me_y // (2 * step) * step + me_y % step
        return pl.ds(pl.multiple_of(at * near, 8), near)

    def copies_a(f, mode, side):
        step, tiles = spread(rows, mode)
        return [
            pltpu.make_async_remote_copy(
                src_ref=send_a.at[f % slots_a, mode, side, u - 1],
                dst_ref=recv_a.at[f, mode, side, :, own_lines(mode)],
                send_sem=send_a_sem.at[f % slots_a],
                recv_sem=recv_a_sem.at[f, mode, side],
                device_id=(flip(me_y, j - side * step), me_z),
                device_id_type=MESH,
            )
            for j, s, u in tiles
            if s == side and u > 0
        ]

    def copy_p(f, mode):
        return pltpu.make_async_remote_copy(
            src_ref=send_p.at[f % slots_p, mode],
            dst_ref=recv_p.at[f, mode],
            send_sem=send_p_sem.at[f % slots_p, mode],
            recv_sem=recv_p_sem.at[f, mode],
            device_id=(flip(me_y, strides[mode]), me_z),
            device_id_type=MESH,
        )

    def copy_b(f, mode, k):
        count = part * rows
        at = me_z * depth + mode * count
        return pltpu.make_async_remote_copy(
            src_ref=send_b.at[
                f % slots_b, pl.ds((me_z + k) % columns * share, share), pl.ds(mode * count, count)
            ],
            dst_ref=recv_b.at[f, :, pl.ds(pl.multiple_of(at, 8), count)],
            send_sem=send_b_sem.at[f % slots_b, mode],
            recv_sem=recv_b_sem.at[f],
            device_id=(me_y, (me_z + k) % columns),
            device_id_type=MESH,
        )

    def free_b(f, mode):
        count = part * rows
        sent = send_b.at[
            f % slots_b, pl.ds(0, (columns - 1) * share), pl.ds(mode * count, count)
        ]
        settle(sent, send_b_sem.at[f % slots_b, mode])

    def copy_c(f, j):
        return pltpu.make_async_remote_copy(
            src_ref=send_c.at[f, pl.ds(flip(me_y, j), 1)],
            dst_ref=recv_c.at[f, pl.ds(me_y, 1)],
            send_sem=send_c_sem.at[0],
            recv_sem=recv_c_sem.at[f],
            device_id=(flip(me_y, j), me_z),
            device_id_type=MESH,
        )

    def copy_z(u, k):
        return pltpu.make_async_remote_copy(
            src_ref=send_z.at[k - 1, pl.ds(2 * u, 2)],
            dst_ref=recv_z.at[pl.ds(2 * u, 2), pl.ds(pl.multiple_of(me_z * depth, 8), depth)],
            send_sem=send_z_sem.at[0],
            recv_sem=recv_z_sem.at[u],
            device_id=(me_y, (me_z + k) % columns),
            device_id_type=MESH,
        )

    def copy_y(j):
        return pltpu.make_async_remote_copy(
            src_ref=send_y.at[flip(me_y, j)],
            dst_ref=recv_y.at[pl.ds(me_y * steps, steps)],
            send_sem=send_y_sem.at[0],
            recv_sem=recv_y_sem.at[0],
            device_id=(flip(me_y, j), me_z),
            device_id_type=MESH,
        )

    def pair_of(f):
        return f // 6 + f // 8, f - 3 - 2 * (f // 6) - f // 8

    def contract_third(f):
        product = f >= 3
        left, right = pair_of(f)
        left = jnp.where(product, left, f)
        right = jnp.where(product, right, f)
        group = lax.broadcasted_iota(jnp.int32, (near, LANES), 1) % rows
        masks = [group == flip(me_y, r) for r in range(rows)]

        def piece(r, carry):
            @pl.when(f < 3)
            def _():
                loaded(f, r)

            value = fine[left, r] * jnp.where(product, fine[right, r], 1.0)
            value = value.reshape(blocks * near, fine_points)
            lines[r] = rows_times(value, third[r]).reshape(blocks, near, LANES)
            return carry

        lax.fori_loop(0, rows, piece, 0)
        for mode in range(2):
            _, tiles = spread(rows, mode)

            def regroup(q, carry):
                parts = [lines[r, mode * part + q] for r in range(rows)]
                for j, side, u in tiles:
                    out = parts[-1]
                    for r in range(rows - 1):
                        out = jnp.where(masks[j ^ r], parts[r], out)
                    if u == 0:
                        recv_a[f, mode, side, q, own_lines(mode)] = out
                    else:
                        send_a[f % slots_a, mode, side, u - 1, q] = out
                return carry

            lax.fori_loop(0, part, regroup, 0)
            if mode == 0:

                @pl.when(f == 0)
                def _():
                    pl.semaphore_wait(barrier, columns + rows - 2)

            for side in (1, 0):
                for copy in copies_a(f, mode, side):
                    copy.start()

    def free_a(f):
        settle(send_a.at[f % slots_a], send_a_sem.at[f % slots_a])

    def arrived_a(f, mode, side):
        others = (rows // 2 - 1) * near
        settle(recv_a.at[f, mode, side, :, pl.ds(0, others)], recv_a_sem.at[f, mode, side])

    def table_times(table, value):
        top, rest = split(value)
        both = dot(table, top)
        return both[:M] + both[M:] + dot(table[:M], rest)

    def partial_first(f, mode, side):
        for at in range(0, part, 2):
            spots = range(at, min(at + 2, part))
            value = jnp.concatenate([recv_a[f, mode, side, q] for q in spots], axis=1)
            out = table_times(first[mode], value)
            for i, q in enumerate(spots):
                yield q, out[:, i * LANES : (i + 1) * LANES]

    def first_out(f):
        for mode in range(2):
            arrived_a(f, mode, 1)

            @pl.when(f >= slots_p)
            def _():
                copy_p(f - slots_p, mode).wait_send()

            for q, out in partial_first(f, mode, 1):
                send_p[f % slots_p, mode, q] = out
            copy_p(f, mode).start()

    def first_in(f):
        slot = f % slots_b
        for mode in range(2):
            arrived_a(f, mode, 0)
            copy_p(f, mode).wait_recv()

            @pl.when(f >= slots_b)
            def _():
                free_b(f - slots_b, mode)

            count = part * rows
            for q, out in partial_first(f, mode, 0):
                out = out + recv_p[f, mode, q]
                send_b[slot, :, pl.ds(mode * count + q * rows, rows)] = out.T.reshape(
                    M // rows, rows, M
                )
            for k in range(1, columns):
                copy_b(f, mode, k).start()
            at = pl.multiple_of(me_z * depth + mode * count, 8)
            recv_b[f, :, pl.ds(at, count)] = send_b[
                slot, pl.ds(me_z * share, share), pl.ds(mode * count, count)
            ]

    def contract_second(f):
        settle(recv_b.at[f, :, pl.ds(0, (columns - 1) * depth)], recv_b_sem.at[f])
        for h in range(share // 2):
            value = jnp.concatenate([recv_b[f, 2 * h + i] for i in range(2)], axis=1)
            out = table_times(second[...], value)
            for i in range(2):
                piece = out[:, i * LANES : (i + 1) * LANES]
                for d in range(rows):
                    send_c[f, d, 2 * h + i] = piece[d * band : (d + 1) * band]
        for j in range(1, rows):
            copy_c(f, j).start()
        recv_c[f, me_y] = send_c[f, me_y]

    def store(f, product):
        source, target, at = (stress, stress_out, f - 3) if product else (filtered, filtered_out, f)
        return pltpu.make_async_copy(source.at[at], target.at[at], out_sem.at[int(product)])

    def place(f, product):
        settle(recv_c.at[f, pl.ds(0, rows - 1)], recv_c_sem.at[f])
        whole = recv_c.at[f].reshape(rows * share * band, M)

        def line(m, carry):
            out = whole[pl.ds(m, block, stride=band), :]
            if product:
                left, right = pair_of(f)
                stress[f - 3, m] = out - filtered[left, m] * filtered[right, m]
            else:
                filtered[f, m] = out
            return carry

        lax.fori_loop(0, band, line, 0)
        store(f, product).start()

    def direct_contract_third(begin, end):
        group = lax.broadcasted_iota(jnp.int32, (depth, LANES), 1) // block
        masks = [group == (me_z + k) % columns for k in range(columns)]
        units = steps // 2

        def unit(u, carry):
            load_natural(u).wait()

            def piece(s, inner):
                value = jnp.concatenate(
                    [natural[u % 2, i * columns + s] for i in range(2)], axis=0
                )
                value = value * value
                direct_lines[s] = rows_times(value, direct_third[s]).reshape(2, depth, LANES)
                return inner

            lax.fori_loop(0, columns, piece, 0)

            @pl.when(u + 2 < units)
            def _():
                load_natural(u + 2).start()

            for i in range(2):
                parts = [direct_lines[s, i] for s in range(columns)]
                for k in range(columns):
                    out = parts[-1]
                    for s in range(columns - 1):
                        out = jnp.where(masks[(k + s) % columns], parts[s], out)
                    if k == 0:
                        recv_z[2 * u + i, pl.ds(pl.multiple_of(me_z * depth, 8), depth)] = out
                    else:
                        send_z[k - 1, 2 * u + i] = out
            for k in range(1, columns):
                copy_z(u, k).start()
            return carry

        lax.fori_loop(begin, end, unit, 0)

    def direct_contract_second():
        def piece(h, carry):
            others = pl.ds(0, (columns - 1) * depth)
            settle(recv_z.at[pl.ds(2 * h, 2), others], recv_z_sem.at[h])
            value = jnp.concatenate([recv_z[2 * h + i] for i in range(2)], axis=1)
            out = table_times(base[...], value)
            for i in range(2):
                for d in range(rows):
                    send_y[d, 2 * h + i] = out[
                        d * band : (d + 1) * band, i * LANES : (i + 1) * LANES
                    ]
            return carry

        lax.fori_loop(0, steps // 2, piece, 0)
        for j in range(1, rows):
            copy_y(j).start()
        recv_y[pl.ds(me_y * steps, steps)] = send_y[me_y]

    def direct_contract_first():
        settle(recv_y.at[pl.ds(0, (rows - 1) * steps)], recv_y_sem.at[0])
        pad = jnp.zeros((LANES - rows * steps, LANES), jnp.float32)
        for m in range(band):
            plane = jnp.concatenate([recv_y[:, m, :], pad], axis=0).T
            for g in range(columns):
                turned[g, m * block : (m + 1) * block] = plane[g * block : (g + 1) * block]
        out = jnp.zeros((band * block, M), jnp.float32)
        for g in range(columns):
            table = direct_first[(g + columns - me_z) % columns]
            out = out + rows_times(turned[g], table)
        out = out.reshape(band, block, M)
        stress[spun - 3] = out - filtered[last_left] * filtered[last_right]
        store(spun, True).start()

    def loop(start, stop, *work):
        def body(f, carry):
            for one in work:
                one(f)
            return carry

        lax.fori_loop(start, stop, body, 0)

    table_copies[0].wait()

    def opening(f):
        contract_third(f)

        @pl.when(f == 0)
        def _():
            for copy in table_copies[1:4]:
                copy.wait()
            settle(first, table_sem.at[4])

        load(f + 1)
        direct_contract_third(f, 1 + f * (steps // 2 - 1))

    loop(0, slots_a, opening)

    points = base.shape[1]
    row = lax.broadcasted_iota(jnp.int32, (points, points), 0)
    column = lax.broadcasted_iota(jnp.int32, (points, points), 1)
    swap = jnp.where(row == flip_by(column, me_y, rows), 1.0, 0.0).astype(jnp.bfloat16)
    second[...] = dot(base[...], swap).astype(jnp.bfloat16)

    def round_of(f):
        first_out(f)

        @pl.when(f >= 1)
        def _():
            first_in(f - 1)

        @pl.when(f + slots_a < spun)
        def _():
            free_a(f)
            contract_third(f + slots_a)

    loop(0, spun - 1, round_of)
    first_out(spun - 1)
    loop(0, spun - 3, contract_second)
    direct_contract_second()
    first_in(spun - 2)
    contract_second(spun - 3)
    first_in(spun - 1)
    loop(0, 3, lambda f: place(f, False))
    contract_second(spun - 2)
    loop(3, spun - 3, lambda f: place(f, True))
    direct_contract_first()
    contract_second(spun - 1)
    loop(spun - 3, spun, lambda f: place(f, True))

    loop(spun - slots_a, spun, free_a)

    def drain_p(f):
        for mode in range(2):
            copy_p(f, mode).wait_send()

    loop(spun - slots_p, spun, drain_p)

    def drain_b(f):
        for mode in range(2):
            free_b(f, mode)

    loop(spun - slots_b, spun, drain_b)

    settle(send_c.at[:, pl.ds(0, rows - 1)], send_c_sem.at[0])
    settle(send_z, send_z_sem.at[0])
    settle(send_y.at[pl.ds(0, rows - 1)], send_y_sem.at[0])
    settle(filtered, out_sem.at[0])
    settle(stress, out_sem.at[1])


def tables(fine, rows, columns):
    matrix = line_filter(fine, M)
    block = M // columns
    share = block // rows
    near = fine // rows
    steps = near // columns
    top, rest = halves(matrix)
    both = np.concatenate([top, rest])
    spot, group = np.arange(M) // rows, np.arange(M) % rows
    third = []
    for r in range(rows):
        order = spot // share * block + (group ^ r) * share + spot % share
        third.append(np.concatenate([top.T[:, order], rest.T[:, order]], axis=1))
    first = []
    for mode in range(2):
        step, _ = spread(rows, mode)
        spots = np.arange(rows // 2)
        for half in range(2):
            peers = spots // step * (2 * step) + half * step + spots % step
            order = (peers[:, None] * near + np.arange(near)).reshape(-1)
            first.append(both[:, order])
    first = np.stack(first).reshape(2, 2, 2 * M, fine // 2)
    direct_third, direct_first = [], []
    for s in range(columns):
        order = np.concatenate(
            [np.arange(block) + (g - s) % columns * block for g in range(columns)]
        )
        direct_third.append(np.concatenate([top.T[:, order], rest.T[:, order]], axis=1))
        points = np.arange(rows * steps) * columns + s
        table = np.concatenate([top.T[points], rest.T[points]], axis=1)
        direct_first.append(np.pad(table, ((0, LANES - rows * steps), (0, 0))))
    return np.stack(third), first, both, np.stack(direct_third), np.stack(direct_first)


def kernel_shards(velocity):
    rows, columns = lax.axis_size("py"), lax.axis_size("pz")
    _, near, depth, fine = velocity.shape
    blocks = depth // rows
    block, band = M // columns, M // rows
    share = block // rows
    half, part, steps = rows // 2, blocks // 2, near // columns
    spun = fields_count - 1
    slots_a, slots_p, slots_b = 2, 2, 2
    constants = tables(fine, rows, columns)
    third, first, base, direct_third, direct_first = constants
    dma = pltpu.SemaphoreType.DMA
    f32, bf16 = jnp.float32, jnp.bfloat16
    return pl.pallas_call(
        functools.partial(kernel, rows, columns),
        out_shape=(
            jax.ShapeDtypeStruct((3, band, block, M), f32),
            jax.ShapeDtypeStruct((6, band, block, M), f32),
        ),
        in_specs=[pl.BlockSpec(memory_space=pl.ANY)] * (1 + len(constants)),
        out_specs=(pl.BlockSpec(memory_space=pl.ANY),) * 2,
        scratch_shapes=[
            pltpu.VMEM((3, band, block, M), f32),
            pltpu.VMEM((6, band, block, M), f32),
            pltpu.VMEM(third.shape, bf16),
            pltpu.VMEM(first.shape[1:], bf16),
            pltpu.VMEM(base.shape, bf16),
            pltpu.VMEM(base.shape, bf16),
            pltpu.VMEM(direct_third.shape, bf16),
            pltpu.VMEM(direct_first.shape, bf16),
            pltpu.VMEM((3, rows, blocks, near, fine), f32),
            pltpu.VMEM((rows, blocks, near, LANES), f32),
            pltpu.VMEM((slots_a, 2, 2, half - 1, part, near, LANES), f32),
            pltpu.VMEM((spun, 2, 2, part, half * near, LANES), f32),
            pltpu.VMEM((slots_p, 2, part, M, LANES), f32),
            pltpu.VMEM((spun, 2, part, M, LANES), f32),
            pltpu.VMEM((slots_b, columns * share, depth, M), f32),
            pltpu.VMEM((spun, share, columns * depth, M), f32),
            pltpu.VMEM((spun, rows, share, band, M), f32),
            pltpu.VMEM((spun, rows, share, band, M), f32),
            pltpu.VMEM((2, 2 * columns, depth, fine), f32),
            pltpu.VMEM((columns, 2, depth, LANES), f32),
            pltpu.VMEM((columns - 1, steps, depth, LANES), f32),
            pltpu.VMEM((steps, columns * depth, LANES), f32),
            pltpu.VMEM((rows, steps, band, LANES), f32),
            pltpu.VMEM((rows * steps, band, LANES), f32),
            pltpu.VMEM((columns, band * block, LANES), f32),
            dma((2,)),
            dma((5,)),
            dma((rows,)),
            dma((2,)),
            dma((slots_a,)),
            dma((spun, 2, 2)),
            dma((slots_p, 2)),
            dma((spun, 2)),
            dma((slots_b, 2)),
            dma((spun,)),
            dma((1,)),
            dma((spun,)),
            dma((1,)),
            dma((steps // 2,)),
            dma((1,)),
            dma((1,)),
        ],
        compiler_params=pltpu.CompilerParams(
            collective_id=0, has_side_effects=True, vmem_limit_bytes=67_000_000
        ),
    )(velocity, *[jnp.asarray(constant) for constant in constants])


def plain_shards(velocity):
    matrix = jnp.asarray(line_filter(velocity.shape[3], M))
    components = [velocity[component] for component in range(3)]
    fields = jnp.stack(components + [components[a] * components[b] for a, b in factor_pairs])
    high = lax.Precision.HIGHEST
    third = jnp.einsum("fabk,mk->fabm", fields, matrix, precision=high)
    third = lax.all_to_all(third, "pz", split_axis=3, concat_axis=2, tiled=True)
    second = jnp.einsum("fabm,nb->fanm", third, matrix, precision=high)
    second = lax.all_to_all(second, "py", split_axis=2, concat_axis=1, tiled=True)
    coarse = jnp.einsum("fanm,pa->fnmp", second, matrix, precision=high)
    stress = jnp.stack(
        [coarse[3 + p] - coarse[a] * coarse[b] for p, (a, b) in enumerate(factor_pairs)]
    )
    return coarse[:3], stress


def shards(velocity):
    rows, columns = lax.axis_size("py"), lax.axis_size("pz")
    _, lines, depth, fine = velocity.shape
    whole_tiles = (
        M == LANES
        and rows % 8 == 0
        and rows & (rows - 1) == 0
        and lines % 8 == 0
        and lines % (2 * columns) == 0
        and depth % (2 * rows) == 0
        and M % (2 * rows * columns) == 0
        and (M // rows) % 8 == 0
        and rows * (lines // columns) <= LANES
    )
    return kernel_shards(velocity) if whole_tiles else plain_shards(velocity)


def solution(mesh):
    placed = P(None, "py", "pz", None)
    return jax.shard_map(
        shards, mesh=mesh, in_specs=(placed,), out_specs=(placed, placed), check_vma=False
    )
```
